128 devices in a mesh: tm: 2 (over z_hi), member: 4 (over y), state: 16 (over z_lo, x, core).
Axes of the slice: x: 4, y: 4, z: 4 (z_hi: 2, z_lo: 2; z = z_hi * 2 + z_lo), core: 2. Of those that a mesh axis runs over, the one named last changes fastest.
Arguments:
- members: bfloat16 [4, 8, 16, 768, 1536], P('tm', 'member', None, 'state'), may hold values from -6 to 6
- slot_grad: float32 [4, 16, 768, 1536], P('tm', None, 'state'), may hold values from -6 to 6
- diffusivity: float32 [768, 1536], P('state'), may hold values from 0.03 to 0.24
- vertical: float32 [16, 16], replicated, may hold values from -0.3 to 2.1, as said below
Outputs:
- control_gradient: float32 [16, 8, 768, 1536], P('tm', 'member', 'state')
The draws below stay inside these ranges and needn't reach their ends.
Inputs may be any that keep to these rules, and one draw needn't show every extreme that they name: `vertical`: the diagonal entries lie between 0.5 and 2.1.
All inputs are finite; a program needn't handle non-finite values.
Results may differ from the reference program's by a relative error of at most 0.0003.
Values sent between devices are 32-bit elements; how exact they have to be, the bound alone decides.
A program may use at most 128 MiB of HBM per device.

```python
import math
import jax
import jax.numpy as jnp
from jax import lax

LON = 1536
LEVELS = 16
NSTEP = 4
LAT = 768
MEMBERS = 8
SLOTS = 4


def draw_vertical(key, part):
    first_key, second_key = jax.random.split(jax.random.fold_in(key, 17))
    offdiag = jnp.clip(jax.random.normal(first_key, (LEVELS, LEVELS), jnp.float32), -3.0, 3.0) / 3.0
    diagonal = jnp.exp(jax.random.uniform(second_key, (LEVELS,), jnp.float32, -0.69, 0.69))
    identity = jnp.eye(LEVELS, dtype=jnp.float32)
    return 0.27 * offdiag * (1.0 - identity) + identity * diagonal[None, :]


def levels(stream_key, shape, pieces, smallest, top_value):
    level, own = 1.0, jax.random.fold_in(stream_key, 6)
    for axis_at, parts in pieces:
        heights = jnp.exp(jax.random.uniform(jax.random.fold_in(own, axis_at), (parts,), jnp.float32, smallest / len(pieces), top_value / len(pieces)))
        level = level * jnp.repeat(heights, shape[axis_at] // parts).reshape([-1 if axis == axis_at else 1 for axis in range(len(shape))])
    return level


def noise(stream_key, shape, width, limit, cuts=(), kind=jnp.bfloat16):
    gain = levels(stream_key, shape, cuts, -0.22, 0.18) if cuts else 1.0
    result = jax.random.normal(stream_key, shape, jnp.float32) * width * gain
    return jnp.minimum(jnp.maximum(result, -limit), limit).astype(kind)


def setup_inputs(seed: int = 0) -> dict:
    key_of = jax.random.split(jax.random.key(seed), 5)
    members = noise(key_of[0], (SLOTS, MEMBERS, LEVELS, LAT, LON), 1.0, 6.0, ((0, 2), (1, 4), (3, 16)))
    slot_grad = noise(key_of[1], (SLOTS, LEVELS, LAT, LON), 1.0, 6.0, ((0, 2), (2, 16)), jnp.float32)
    diffusivity = jnp.clip(jnp.exp(math.log(0.24) - 2.0794415 * jax.random.uniform(key_of[2], (LAT, LON), jnp.float32) ** levels(key_of[2], (LAT, LON), ((0, 16),), -0.2, 0.2)), 0.03, 0.24)
    vertical = draw_vertical(jax.random.fold_in(key_of[4], 71), 0)
    return dict(members=members, slot_grad=slot_grad, diffusivity=diffusivity, vertical=vertical)


def stencil_update(centre, spread):
    middle = spread[..., 1:-1, :]
    return centre + spread[..., 2:, :] + spread[..., :-2, :] + jnp.roll(middle, 1, -1) + jnp.roll(middle, -1, -1) - 4.0 * middle


def reference(members, slot_grad, diffusivity, vertical):
    ensemble = members.shape[1]
    spread_scale = float(ensemble - 1) ** -0.5
    centre = jnp.sum(members, axis=1, dtype=jnp.float32) / ensemble

    def member_product(which):
        single = lax.dynamic_index_in_dim(members, which, 1, keepdims=False).astype(jnp.float32)
        perturbed = (single - centre) * spread_scale
        return jnp.sum(perturbed * slot_grad, axis=0)

    partial_value = lax.map(member_product, jnp.arange(ensemble, dtype=jnp.int32))
    field = jnp.einsum("ml,kmab->lkab", vertical, partial_value, precision=lax.Precision.HIGHEST)
    for step_index in range(NSTEP):
        spread = jnp.pad(diffusivity * field, ((0, 0), (0, 0), (1, 1), (0, 0)))
        field = stencil_update(field, spread)
    return field
```

```python
import functools

import jax
import jax.numpy as jnp
from jax import lax
from jax.experimental import pallas as pl
from jax.experimental.pallas import tpu as pltpu
from jax.sharding import PartitionSpec as P

NSTEP = 4
MESH = pl.DeviceIdType.MESH
LANES = 128


def kernel(
    members, slot_grad, diffusivity, vertical, out,
    mv, gv, cs, co, zr, rb, ps, rsr, sg, kp, hst, hsb, hrt, hrb, w, v,
    ld_sem, kp_sem, z_s, z_r, ref_s, ref_r, rs_s, rs_r, ag_s, ag_r, h_s, h_r,
    *, n_state, scale, n_members,
):
    f32 = jnp.float32
    tm, mb, st = lax.axis_index("tm"), lax.axis_index("member"), lax.axis_index("state")
    levels = mv.shape[3]
    half = levels // 2
    quarter = mv.shape[-1]
    tiles = quarter // LANES
    zpeer = (1 - tm, mb, st)
    up, down = (tm, mb, st - 1), (tm, mb, st + 1)
    has_up, has_down = st > 0, st < n_state - 1

    def turn(i):
        return lax.rem(mb + i, 4)

    def ypeer(i):
        return (tm, turn(i), st)

    def remote(src, dst, send, recv, peer):
        return pltpu.make_async_remote_copy(
            src_ref=src, dst_ref=dst, send_sem=send, recv_sem=recv, device_id=peer, device_id_type=MESH
        )

    def block(j):
        rows = lax.rem(2 * (j // 4), 3) * 16
        q = turn(lax.rem(j, 4))
        return pl.multiple_of(rows, 16), q

    def loads(j):
        r0, q = block(j)
        c0 = pl.multiple_of(q * quarter, LANES)
        return (
            pltpu.make_async_copy(
                members.at[:, :, :, pl.ds(r0, 16), pl.ds(c0, quarter)], mv.at[j], ld_sem.at[j, 0]
            ),
            pltpu.make_async_copy(
                slot_grad.at[:, :, pl.ds(r0, 16), pl.ds(c0, quarter)], gv.at[j], ld_sem.at[j, 1]
            ),
        )

    def start_loads(j, c):
        for copy in loads(j):
            copy.start()
        return c

    lax.fori_loop(0, 12, start_loads, 0)
    kload = pltpu.make_async_copy(diffusivity, kp.at[pl.ds(8, 48)], kp_sem)
    kload.start()

    barrier = pltpu.get_barrier_semaphore()
    pl.semaphore_signal(barrier, inc=1, device_id=zpeer, device_id_type=MESH)
    for i in (1, 2, 3):
        pl.semaphore_signal(barrier, inc=1, device_id=ypeer(i), device_id_type=MESH)

    @pl.when(has_up)
    def _():
        pl.semaphore_signal(barrier, inc=1, device_id=up, device_id_type=MESH)

    @pl.when(has_down)
    def _():
        pl.semaphore_signal(barrier, inc=1, device_id=down, device_id_type=MESH)

    zr[mb, :, 1] = jnp.zeros(zr.shape[1:2] + zr.shape[3:], f32)
    w[pl.ds(0, 8)] = jnp.zeros((8, w.shape[1]), f32)
    w[pl.ds(56, 8)] = jnp.zeros((8, w.shape[1]), f32)

    def z_edge(j, count):
        r0, q = block(j)
        rows, ks = pl.ds(r0, 16), pl.ds(0, count)
        return remote(cs.at[q, :, ks, rows], zr.at[q, :, ks, rows], z_s.at[j], z_r.at[j], zpeer)

    def z_mid(l, i):
        q, rows, n = turn(i), pl.ds(16, 16), 8 + 4 * l + i
        ks = pl.ds(0, 1) if i == 0 else pl.ds(0, 2)
        return remote(cs.at[q, l, ks, rows], zr.at[q, l, ks, rows], z_s.at[n], z_r.at[n], zpeer)

    def ref_copy(s, i):
        r0 = pl.multiple_of(lax.rem(2 * s, 3) * 16, 16)
        src = cs.at[mb, :, 1, pl.ds(r0, 16)]
        return remote(src, rb.at[mb, :, pl.ds(r0, 16)], ref_s.at[s, i - 1], ref_r.at[s, i - 1], ypeer(4 - i))

    def span(u):
        if isinstance(u, int) and u < 2:
            return pl.ds(0, half), pl.ds(32 * u, 16)
        return pl.ds(u - 2, 1), pl.ds(16, 16)

    def rs_copy(u, i):
        lv, rows = span(u)
        q = turn(i)
        return remote(ps.at[q, lv, rows], rsr.at[i - 1, lv, rows], rs_s.at[u, i - 1], rs_r.at[u, i - 1], ypeer(i))

    def ag_copy(u, i):
        lv, rows = span(u)
        here = sg.at[mb, lv, rows]
        return remote(here, here, ag_s.at[u, i - 1], ag_r.at[u, i - 1], ypeer(i))

    def k_up():
        return remote(kp.at[pl.ds(8, 8)], kp.at[pl.ds(56, 8)], h_s.at[0], h_r.at[0], up)

    def k_down():
        return remote(kp.at[pl.ds(48, 8)], kp.at[pl.ds(0, 8)], h_s.at[1], h_r.at[1], down)

    def f_up():
        return remote(hst, hrb, h_s.at[2], h_r.at[2], up)

    def f_down():
        return remote(hsb, hrt, h_s.at[3], h_r.at[3], down)

    def products(j):
        r0, q = block(j)
        rows = pl.ds(r0, 16)
        own = half * tm
        other = half - own

        def tile(n, c):
            k = lax.rem(n, 2)
            lanes = pl.ds(pl.multiple_of((n // 2) * LANES, LANES), LANES)
            part = [
                mv[j, 0, k, m, :, lanes].astype(f32) * gv[j, 0, m, :, lanes]
                + mv[j, 1, k, m, :, lanes].astype(f32) * gv[j, 1, m, :, lanes]
                for m in range(levels)
            ]
            for start, dst in ((other, cs), (own, co)):
                for l in range(half):
                    total = vertical[0, start + l] * part[0]
                    for m in range(1, levels):
                        total = total + vertical[m, start + l] * part[m]
                    dst[q, l, k, rows, lanes] = total
            return c

        lax.fori_loop(0, 2 * tiles, tile, 0)

    def step(j, c):
        r0, q = block(j)
        rows = pl.ds(r0, 16)
        s, i = j // 4, lax.rem(j, 4)
        for copy in loads(j):
            copy.wait()
        products(j)

        @pl.when(j == 0)
        def _():
            pl.semaphore_wait(barrier, 4 + has_up.astype(jnp.int32) + has_down.astype(jnp.int32))

        @pl.when(i == 0)
        def _():
            for n in (1, 2, 3):
                ref_copy(s, n).start()

            def sub(l, c):
                cs[q, l, 0, rows] = cs[q, l, 0, rows] - cs[q, l, 1, rows]
                return c

            lax.fori_loop(0, half, sub, 0)

            @pl.when(s < 2)
            def _():
                z_edge(j, 1).start()

        @pl.when(i > 0)
        def _():
            pltpu.make_async_remote_copy(
                src_ref=rb.at[q, :, rows], dst_ref=rb.at[q, :, rows],
                send_sem=ref_s.at[s, i - 1], recv_sem=ref_r.at[s, i - 1],
                device_id=zpeer, device_id_type=MESH,
            ).wait_recv()

            def sub(l, c):
                ref = rb[q, l, rows]
                cs[q, l, 0, rows] = cs[q, l, 0, rows] - ref
                cs[q, l, 1, rows] = cs[q, l, 1, rows] - ref
                return c

            lax.fori_loop(0, half, sub, 0)

            @pl.when(s < 2)
            def _():
                z_edge(j, 2).start()

        return c

    lax.fori_loop(0, 12, step, 0)

    kload.wait()

    @pl.when(has_up)
    def _():
        k_up().start()

    @pl.when(has_down)
    def _():
        k_down().start()

    @pl.when(jnp.logical_not(has_up))
    def _():
        kp[pl.ds(0, 8)] = jnp.zeros((8, kp.shape[1]), f32)
        hrt[...] = jnp.zeros(hrt.shape, f32)

    @pl.when(jnp.logical_not(has_down))
    def _():
        kp[pl.ds(56, 8)] = jnp.zeros((8, kp.shape[1]), f32)
        hrb[...] = jnp.zeros(hrb.shape, f32)

    def add_up(q, l, rows):
        a = co[q, l, 0, rows] + zr[q, l, 0, rows]
        b = co[q, l, 1, rows] + zr[q, l, 1, rows]
        co[q, l, 0, rows] = a
        co[q, l, 1, rows] = b
        ps[q, l, rows] = a + b

    def arrive_edge(u, i):
        z_edge(4 * u + i, 2 if i else 1).wait_recv()
        q = turn(i)

        def body(l, c):
            add_up(q, l, pl.ds(32 * u, 16))
            return c

        lax.fori_loop(0, half, body, 0)
        if i:
            rs_copy(u, i).start()

    def arrive_mid(l):
        for i in range(4):
            z_mid(l, i).wait_recv()
            add_up(turn(i), l, pl.ds(16, 16))
            if i:
                rs_copy(2 + l, i).start()

    def total(u):
        lv, rows = span(u)
        for i in (1, 2, 3):
            rs_copy(u, i).wait_recv()

        def body(l, c):
            sg[mb, l, rows] = (ps[mb, l, rows] + rsr[0, l, rows]) + (rsr[1, l, rows] + rsr[2, l, rows])
            return c

        lax.fori_loop(lv.start, lv.start + lv.size, body, 0)
        for i in (1, 2, 3):
            ag_copy(u, i).start()

    def centred(u):
        lv, rows = span(u)
        for i in (1, 2, 3):
            q = turn(i)
            pltpu.make_async_remote_copy(
                src_ref=sg.at[q, lv, rows], dst_ref=sg.at[q, lv, rows],
                send_sem=ag_s.at[u, 3 - i], recv_sem=ag_r.at[u, 3 - i],
                device_id=zpeer, device_id_type=MESH,
            ).wait_recv()

        def body(l, c):
            for q in range(4):
                mean = sg[q, l, rows] * (1.0 / n_members)
                for k in range(2):
                    out[l, k, rows, pl.ds(q * quarter, quarter)] = (co[q, l, k, rows] - mean) * scale
            return c

        lax.fori_loop(lv.start, lv.start + lv.size, body, 0)

    def edge_top():
        def body(l, c):
            for k in range(2):
                hst[l, pl.ds(4 * k, 4)] = out[l, k, pl.ds(0, 4)]
            return c

        @pl.when(has_up)
        def _():
            lax.fori_loop(0, half, body, 0)
            f_up().start()

    def edge_bottom():
        def body(l, c):
            for k in range(2):
                hsb[l, pl.ds(4 * k, 4)] = out[l, k, pl.ds(44, 4)]
            return c

        @pl.when(has_down)
        def _():
            lax.fori_loop(0, half, body, 0)
            f_down().start()

    def smooth(l):
        for k in range(2):
            w[pl.ds(8, 48)] = out[l, k]
            w[pl.ds(4, 4)] = hrt[l, pl.ds(4 * k, 4)]
            w[pl.ds(56, 4)] = hrb[l, pl.ds(4 * k, 4)]

            def filter_step(n, c):
                for t in range(8):
                    v[pl.ds(8 * t + 8, 8)] = kp[pl.ds(8 * t, 8)] * w[pl.ds(8 * t, 8)]
                for t in range(8):
                    mid = v[pl.ds(8 * t + 8, 8)]
                    around = v[pl.ds(8 * t + 9, 8)] + v[pl.ds(8 * t + 7, 8)]
                    around = around + (pltpu.roll(mid, 1, 1) + pltpu.roll(mid, mid.shape[1] - 1, 1))
                    w[pl.ds(8 * t, 8)] = (w[pl.ds(8 * t, 8)] - 4.0 * mid) + around
                return c

            lax.fori_loop(0, NSTEP, filter_step, 0)
            out[l, k] = w[pl.ds(8, 48)]

    def wait_halos():
        @pl.when(has_up)
        def _():
            k_down().wait_recv()
            f_down().wait_recv()

        @pl.when(has_down)
        def _():
            k_up().wait_recv()
            f_up().wait_recv()

    v[pl.ds(0, 8)] = jnp.zeros((8, v.shape[1]), f32)
    v[pl.ds(72, 8)] = jnp.zeros((8, v.shape[1]), f32)

    def start_mid(l):
        for i in range(4):
            z_mid(l, i).start()

    for i in range(4):
        start_mid(i)
        arrive_edge(0, i)
    start_mid(4)
    arrive_edge(1, 0)
    total(0)
    start_mid(5)
    arrive_edge(1, 1)
    centred(0)
    edge_top()
    start_mid(6)
    arrive_edge(1, 2)
    start_mid(7)
    arrive_edge(1, 3)
    arrive_mid(0)
    total(1)
    arrive_mid(1)
    centred(1)
    edge_bottom()
    total(2)
    wait_halos()

    def rest(l, c):
        arrive_mid(l)
        total(l + 1)
        centred(l)
        smooth(l - 2)
        return c

    lax.fori_loop(2, half, rest, 0)
    total(half + 1)
    centred(half)
    smooth(half - 2)
    centred(half + 1)
    smooth(half - 1)

    for j in range(8):
        z_edge(j, 2 if j % 4 else 1).wait_send()

    def sent(l, c):
        for i in range(4):
            z_mid(l, i).wait_send()
        return c

    lax.fori_loop(0, half, sent, 0)
    for i in (1, 2, 3):
        for s in range(3):
            ref_copy(s, i).wait_send()
        for u in (0, 1):
            rs_copy(u, i).wait_send()
            ag_copy(u, i).wait_send()

    def sums_sent(u, c):
        for i in (1, 2, 3):
            rs_copy(u, i).wait_send()
            ag_copy(u, i).wait_send()
        return c

    lax.fori_loop(2, half + 2, sums_sent, 0)

    @pl.when(has_up)
    def _():
        k_up().wait_send()
        f_up().wait_send()

    @pl.when(has_down)
    def _():
        k_down().wait_send()
        f_down().wait_send()


def body(members, slot_grad, diffusivity, vertical, *, sizes):
    slots, pair, levels, rows, lon = members.shape
    half, quarter = levels // sizes["tm"], lon // 4
    n_members = pair * sizes["member"]
    dma = pltpu.SemaphoreType.DMA
    f32 = jnp.float32
    field = (4, half, pair, rows, quarter)
    one = (4, half, rows, quarter)
    scratch = [
        pltpu.VMEM((12, slots, pair, levels, 16, quarter), members.dtype),
        pltpu.VMEM((12, slots, levels, 16, quarter), f32),
        pltpu.VMEM(field, f32),
        pltpu.VMEM(field, f32),
        pltpu.VMEM(field, f32),
        pltpu.VMEM(one, f32),
        pltpu.VMEM(one, f32),
        pltpu.VMEM((3,) + one[1:], f32),
        pltpu.VMEM(one, f32),
        pltpu.VMEM((64, lon), f32),
        pltpu.VMEM((half, 8, lon), f32),
        pltpu.VMEM((half, 8, lon), f32),
        pltpu.VMEM((half, 8, lon), f32),
        pltpu.VMEM((half, 8, lon), f32),
        pltpu.VMEM((64, lon), f32),
        pltpu.VMEM((80, lon), f32),
        dma((12, 2)),
        dma,
        dma((8 + 4 * half,)),
        dma((8 + 4 * half,)),
        dma((3, 3)),
        dma((3, 3)),
        dma((half + 2, 3)),
        dma((half + 2, 3)),
        dma((half + 2, 3)),
        dma((half + 2, 3)),
        dma((4,)),
        dma((4,)),
    ]
    hbm = pl.BlockSpec(memory_space=pl.ANY)
    return pl.pallas_call(
        functools.partial(
            kernel, n_state=sizes["state"], scale=float(n_members - 1) ** -0.5, n_members=n_members
        ),
        out_shape=jax.ShapeDtypeStruct((half, pair, rows, lon), f32),
        in_specs=[hbm, hbm, hbm, pl.BlockSpec(memory_space=pltpu.SMEM)],
        out_specs=pl.BlockSpec(memory_space=pltpu.VMEM),
        scratch_shapes=scratch,
        compiler_params=pltpu.CompilerParams(
            collective_id=0, has_side_effects=True, vmem_limit_bytes=VMEM_LIMIT
        ),
    )(members, slot_grad, diffusivity, vertical)


VMEM_LIMIT = 56 * 1024 * 1024


def solution(mesh):
    in_specs = (
        P("tm", "member", None, "state", None),
        P("tm", None, "state", None),
        P("state", None),
        P(),
    )
    out_specs = P("tm", "member", "state", None)
    step = functools.partial(body, sizes=dict(mesh.shape))
    return jax.shard_map(step, mesh=mesh, in_specs=in_specs, out_specs=out_specs, check_vma=False)
```

```python
import functools

import jax
import jax.numpy as jnp
from jax import lax
from jax.experimental import pallas as pl
from jax.experimental.pallas import tpu as pltpu
from jax.sharding import PartitionSpec as P

NSTEP = 4
MESH = pl.DeviceIdType.MESH
LANES = 128


def kernel(
    members, slot_grad, diffusivity, matrix, out,
    vertical, pp, pr, pg, mv, gv, cs, co, zr, rb, ps, rsr, sg, kp, hst, hsb, hrt, hrb, w, v,
    v_sem, pre_rs_s, pre_rs_r, pre_ag_s, pre_ag_r, ld_sem, kp_sem, z_s, z_r, ref_s, ref_r, rs_s, rs_r, ag_s, ag_r, h_s, h_r,
    *, n_state, scale, n_members,
):
    f32 = jnp.float32
    tm, mb, st = lax.axis_index("tm"), lax.axis_index("member"), lax.axis_index("state")
    levels = mv.shape[3]
    half = levels // 2
    last = half - 1
    mid = pl.ds(8, 32)
    quarter = mv.shape[-1]
    tiles = quarter // LANES
    zpeer = (1 - tm, mb, st)
    up, down = (tm, mb, st - 1), (tm, mb, st + 1)
    has_up, has_down = st > 0, st < n_state - 1

    def turn(i):
        return lax.rem(mb + i, 4)

    def ypeer(i):
        return (tm, turn(i), st)

    def remote(src, dst, send, recv, peer):
        return pltpu.make_async_remote_copy(
            src_ref=src, dst_ref=dst, send_sem=send, recv_sem=recv, device_id=peer, device_id_type=MESH
        )

    block_rows = (0, 32, 16)

    def loads(s, i):
        rows = pl.ds(block_rows[s], 16)
        lanes = pl.ds(pl.multiple_of(turn(i) * quarter, LANES), quarter)
        j = 4 * s + i
        return (
            pltpu.make_async_copy(members.at[:, :, :, rows, lanes], mv.at[j], ld_sem.at[j, 0]),
            pltpu.make_async_copy(slot_grad.at[:, :, rows, lanes], gv.at[j], ld_sem.at[j, 1]),
        )

    def start_loads(s, i):
        for copy in loads(s, i):
            copy.start()

    vload = pltpu.make_async_copy(matrix, vertical, v_sem)
    vload.start()
    start_loads(0, 0)
    start_loads(0, 1)

    barrier = pltpu.get_barrier_semaphore()
    pl.semaphore_signal(barrier, inc=1, device_id=zpeer, device_id_type=MESH)
    for i in (1, 2, 3):
        pl.semaphore_signal(barrier, inc=1, device_id=ypeer(i), device_id_type=MESH)

    @pl.when(has_up)
    def _():
        pl.semaphore_signal(barrier, inc=1, device_id=up, device_id_type=MESH)

    @pl.when(has_down)
    def _():
        pl.semaphore_signal(barrier, inc=1, device_id=down, device_id_type=MESH)

    kload = pltpu.make_async_copy(diffusivity, kp.at[pl.ds(8, 48)], kp_sem)
    kload.start()
    start_loads(0, 2)

    def z_edge(u, i):
        q, rows = turn(i), pl.ds(40 * u, 8)
        ks = pl.ds(0, 1 if u == 1 and isinstance(i, int) and i == 0 else 2)
        n = 4 * u + i
        return remote(cs.at[q, :, ks, rows], zr.at[q, :, ks, rows], z_s.at[n], z_r.at[n], zpeer)

    def z_mid(l, i):
        q, n = turn(i), 8 + 4 * l + i
        ks = pl.ds(0, 1) if i == 0 else pl.ds(0, 2)
        return remote(cs.at[q, l, ks, mid], zr.at[q, l, ks, mid], z_s.at[n], z_r.at[n], zpeer)

    def z_last(k):
        n = 8 + 4 * last + k
        return remote(cs.at[:, last, k, mid], zr.at[:, last, k, mid], z_s.at[n], z_r.at[n], zpeer)

    ref_part = ((pl.ds(0, last), pl.ds(8, 8)), (pl.ds(0, half), pl.ds(32, 16)), (pl.ds(0, last), pl.ds(16, 16)))

    def ref_copy(s, i):
        lv, rows = ref_part[s]
        return remote(
            cs.at[mb, lv, 1, rows], rb.at[mb, lv, rows], ref_s.at[s, i - 1], ref_r.at[s, i - 1], ypeer(4 - i)
        )

    def ref_arrival(s, i):
        lv, rows = ref_part[s]
        here = rb.at[turn(i), lv, rows]
        return remote(here, here, ref_s.at[s, i - 1], ref_r.at[s, i - 1], zpeer)

    def span(u):
        if isinstance(u, int) and u < 2:
            return pl.ds(0, half), pl.ds(40 * u, 8)
        return pl.ds(u - 2, 1), mid

    def rs_copy(u, i):
        lv, rows = span(u)
        q = turn(i)
        return remote(ps.at[q, lv, rows], rsr.at[i - 1, lv, rows], rs_s.at[u, i - 1], rs_r.at[u, i - 1], ypeer(i))

    def ag_copy(u, i):
        lv, rows = span(u)
        here = sg.at[mb, lv, rows]
        return remote(here, here, ag_s.at[u, i - 1], ag_r.at[u, i - 1], ypeer(i))

    def pre_rs(i):
        return remote(pp.at[turn(i)], pr.at[i - 1], pre_rs_s.at[i - 1], pre_rs_r.at[i - 1], ypeer(i))

    def pre_ag(i):
        return remote(pg.at[mb], pg.at[mb], pre_ag_s.at[i - 1], pre_ag_r.at[i - 1], ypeer(i))

    def k_up():
        return remote(kp.at[pl.ds(8, 8)], kp.at[pl.ds(56, 8)], h_s.at[0], h_r.at[0], up)

    def k_down():
        return remote(kp.at[pl.ds(48, 8)], kp.at[pl.ds(0, 8)], h_s.at[1], h_r.at[1], down)

    def f_up():
        return remote(hst, hrb, h_s.at[2], h_r.at[2], up)

    def f_down():
        return remote(hsb, hrt, h_s.at[3], h_r.at[3], down)

    def products(s, i):
        j, q = 4 * s + i, turn(i)
        rows = pl.ds(block_rows[s], 16)
        own = half * tm
        other = half - own

        def tile(n, c):
            k = lax.rem(n, 2)
            lanes = pl.ds(pl.multiple_of((n // 2) * LANES, LANES), LANES)
            part = [
                mv[j, 0, k, m, :, lanes].astype(f32) * gv[j, 0, m, :, lanes]
                + mv[j, 1, k, m, :, lanes].astype(f32) * gv[j, 1, m, :, lanes]
                for m in range(levels)
            ]
            for start, dst in ((other, cs), (own, co)):
                for l in range(half):
                    total = vertical[0, start + l] * part[0]
                    for m in range(1, levels):
                        total = total + vertical[m, start + l] * part[m]
                    dst[q, l, k, rows, lanes] = total
            return c

        lax.fori_loop(0, 2 * tiles, tile, 0)

    ref_tiles = (((8, last),), ((32, last), (40, half)), ((16, last), (24, last)))

    def subtract(s, q, refer, ks):
        for r, count in ref_tiles[s]:
            rows = pl.ds(r, 8)

            def sub(l, c):
                ref = refer(l, rows)
                for k in ks:
                    cs[q, l, k, rows] = cs[q, l, k, rows] - ref
                return c

            lax.fori_loop(0, count, sub, 0)

    def mix(s):
        def step(i, c):
            for ahead in range(4):
                at, to = (s, ahead + 3) if ahead == 0 else (s + 1, ahead - 1)
                if at < 3:

                    @pl.when(i == ahead)
                    def _():
                        start_loads(at, to)

            for copy in loads(s, i):
                copy.wait()
            products(s, i)
            if s == 0:

                @pl.when(i == 0)
                def _():
                    peers = 4 + has_up.astype(jnp.int32) + has_down.astype(jnp.int32)
                    pl.semaphore_wait(barrier, peers)

                z_edge(0, i).start()

            @pl.when(i == 0)
            def _():
                for n in (1, 2, 3):
                    ref_copy(s, n).start()
                subtract(s, mb, lambda l, rows: cs[mb, l, 1, rows], (0,))
                if s == 1:
                    z_edge(1, 0).start()

            return c

        lax.fori_loop(0, 4, step, 0)

    def refer(s):
        def step(i, c):
            q = turn(i)
            ref_arrival(s, i).wait_recv()
            subtract(s, q, lambda l, rows: rb[q, l, rows], (0, 1))
            if s == 1:
                z_edge(1, i).start()
            return c

        lax.fori_loop(1, 4, step, 0)

    vload.wait()
    for s in range(3):
        mix(s)
    for s in (1, 0, 2):
        refer(s)

    kload.wait()

    @pl.when(has_up)
    def _():
        k_up().start()

    @pl.when(has_down)
    def _():
        k_down().start()

    @pl.when(jnp.logical_not(has_up))
    def _():
        kp[pl.ds(0, 8)] = jnp.zeros((8, kp.shape[1]), f32)
        hrt[...] = jnp.zeros(hrt.shape, f32)

    @pl.when(jnp.logical_not(has_down))
    def _():
        kp[pl.ds(56, 8)] = jnp.zeros((8, kp.shape[1]), f32)
        hrb[...] = jnp.zeros(hrb.shape, f32)

    def add_up(q, l, rows):
        a = co[q, l, 0, rows] + zr[q, l, 0, rows]
        b = co[q, l, 1, rows] + zr[q, l, 1, rows]
        co[q, l, 0, rows] = a
        co[q, l, 1, rows] = b
        ps[q, l, rows] = a + b

    def arrive_edge(u, i):
        z_edge(u, i).wait_recv()
        q = turn(i)

        def body(l, c):
            add_up(q, l, pl.ds(40 * u, 8))
            return c

        lax.fori_loop(0, half, body, 0)
        if i:
            rs_copy(u, i).start()

    def arrive_mid(l):
        for i in range(4):
            z_mid(l, i).wait_recv()
            add_up(turn(i), l, mid)
            if i:
                rs_copy(2 + l, i).start()

    def total(u):
        lv, rows = span(u)
        for i in (1, 2, 3):
            rs_copy(u, i).wait_recv()

        def body(l, c):
            sg[mb, l, rows] = (ps[mb, l, rows] + rsr[0, l, rows]) + (rsr[1, l, rows] + rsr[2, l, rows])
            return c

        lax.fori_loop(lv.start, lv.start + lv.size, body, 0)
        for i in (1, 2, 3):
            ag_copy(u, i).start()

    def centred(u):
        lv, rows = span(u)
        for i in (1, 2, 3):
            q = turn(i)
            pltpu.make_async_remote_copy(
                src_ref=sg.at[q, lv, rows], dst_ref=sg.at[q, lv, rows],
                send_sem=ag_s.at[u, 3 - i], recv_sem=ag_r.at[u, 3 - i],
                device_id=zpeer, device_id_type=MESH,
            ).wait_recv()

        def body(l, c):
            for q in range(4):
                mean = sg[q, l, rows] * (1.0 / n_members)
                for k in range(2):
                    out[l, k, rows, pl.ds(q * quarter, quarter)] = (co[q, l, k, rows] - mean) * scale
            return c

        lax.fori_loop(lv.start, lv.start + lv.size, body, 0)

    def pre_sum():
        for n in range(4):
            q = turn(n)
            for h, src in enumerate((cs, co)):
                pp[q, h] = src[q, last, 0, mid] + src[q, last, 1, mid]
            if n:
                pre_rs(n).start()

    def pre_total():
        for i in (1, 2, 3):
            pre_rs(i).wait_recv()
        for h in range(2):
            pg[mb, h] = (pp[mb, h] + pr[0, h]) + (pr[1, h] + pr[2, h])
        for i in (1, 2, 3):
            pre_ag(i).start()

    def pre_centred():
        for i in (1, 2, 3):
            here = pg.at[turn(i)]
            remote(here, here, pre_ag_s.at[3 - i], pre_ag_r.at[3 - i], zpeer).wait_recv()
            ref_copy(1, i).wait_send()
        for q in range(4):
            for h, dst in enumerate((cs, co)):
                mean = pg[q, h] * (1.0 / n_members)
                for k in range(2):
                    dst[q, last, k, mid] = dst[q, last, k, mid] - mean

    def arrive_last(k):
        z_last(k).wait_recv()
        for q in range(4):
            out[last, k, mid, pl.ds(q * quarter, quarter)] = (co[q, last, k, mid] + zr[q, last, k, mid]) * scale

    def edge_top():
        def body(l, c):
            for k in range(2):
                hst[l, pl.ds(4 * k, 4)] = out[l, k, pl.ds(0, 4)]
            return c

        @pl.when(has_up)
        def _():
            lax.fori_loop(0, half, body, 0)
            f_up().start()

    def edge_bottom():
        def body(l, c):
            for k in range(2):
                hsb[l, pl.ds(4 * k, 4)] = out[l, k, pl.ds(44, 4)]
            return c

        @pl.when(has_down)
        def _():
            lax.fori_loop(0, half, body, 0)
            f_down().start()

    def smooth(l, ks=(0, 1)):
        for k in ks:
            w[pl.ds(8, 48)] = out[l, k]
            w[pl.ds(4, 4)] = hrt[l, pl.ds(4 * k, 4)]
            w[pl.ds(56, 4)] = hrb[l, pl.ds(4 * k, 4)]

            def filter_step(n, c):
                for t in range(8):
                    v[pl.ds(8 * t + 8, 8)] = kp[pl.ds(8 * t, 8)] * w[pl.ds(8 * t, 8)]
                for t in range(8):
                    mid = v[pl.ds(8 * t + 8, 8)]
                    around = v[pl.ds(8 * t + 9, 8)] + v[pl.ds(8 * t + 7, 8)]
                    around = around + (pltpu.roll(mid, 1, 1) + pltpu.roll(mid, mid.shape[1] - 1, 1))
                    w[pl.ds(8 * t, 8)] = (w[pl.ds(8 * t, 8)] - 4.0 * mid) + around
                return c

            lax.fori_loop(0, NSTEP, filter_step, 0)
            out[l, k] = w[pl.ds(8, 48)]

    def wait_halos():
        @pl.when(has_up)
        def _():
            k_down().wait_recv()
            f_down().wait_recv()

        @pl.when(has_down)
        def _():
            k_up().wait_recv()
            f_up().wait_recv()

    w[pl.ds(0, 8)] = jnp.zeros((8, w.shape[1]), f32)
    w[pl.ds(56, 8)] = jnp.zeros((8, w.shape[1]), f32)
    zr[mb, pl.ds(0, last), 1, pl.ds(8, 40)] = jnp.zeros((last, 40, quarter), f32)
    zr[mb, last, 1, pl.ds(40, 8)] = jnp.zeros((8, quarter), f32)
    v[pl.ds(0, 8)] = jnp.zeros((8, v.shape[1]), f32)
    v[pl.ds(72, 8)] = jnp.zeros((8, v.shape[1]), f32)

    def start_mid(l):
        for i in range(4):
            z_mid(l, i).start()

    pre_sum()
    start_mid(0)
    start_mid(1)
    for i in range(4):
        arrive_edge(0, i)
    start_mid(2)
    pre_total()
    arrive_edge(1, 0)
    total(0)
    start_mid(3)
    arrive_edge(1, 1)
    pre_centred()
    arrive_edge(1, 2)
    centred(0)
    edge_top()
    start_mid(4)
    arrive_edge(1, 3)
    start_mid(5)
    arrive_mid(0)
    start_mid(6)
    z_last(0).start()
    z_last(1).start()
    total(1)
    total(2)
    centred(1)
    edge_bottom()

    def rest(l, c):
        arrive_mid(l)

        @pl.when(l == 1)
        def _():
            wait_halos()

        centred(l + 1)
        smooth(l - 1)
        total(l + 2)
        return c

    lax.fori_loop(1, last, rest, 0)
    arrive_last(0)
    smooth(last, (0,))
    centred(last + 1)
    smooth(last - 1)
    arrive_last(1)
    smooth(last, (1,))

    for u in range(2):
        for i in range(4):
            z_edge(u, i).wait_send()
    for k in range(2):
        z_last(k).wait_send()

    def sent(l, c):
        for i in range(4):
            z_mid(l, i).wait_send()
        return c

    lax.fori_loop(0, last, sent, 0)
    for i in (1, 2, 3):
        pre_rs(i).wait_send()
        pre_ag(i).wait_send()
        for s in (0, 2):
            ref_copy(s, i).wait_send()
        for u in (0, 1):
            rs_copy(u, i).wait_send()
            ag_copy(u, i).wait_send()

    def sums_sent(u, c):
        for i in (1, 2, 3):
            rs_copy(u, i).wait_send()
            ag_copy(u, i).wait_send()
        return c

    lax.fori_loop(2, last + 2, sums_sent, 0)

    @pl.when(has_up)
    def _():
        k_up().wait_send()
        f_up().wait_send()

    @pl.when(has_down)
    def _():
        k_down().wait_send()
        f_down().wait_send()


def body(members, slot_grad, diffusivity, vertical, *, sizes):
    slots, pair, levels, rows, lon = members.shape
    half, quarter = levels // sizes["tm"], lon // 4
    n_members = pair * sizes["member"]
    dma = pltpu.SemaphoreType.DMA
    f32 = jnp.float32
    field = (4, half, pair, rows, quarter)
    one = (4, half, rows, quarter)
    scratch = [
        pltpu.SMEM((levels, levels), f32),
        pltpu.VMEM((4, 2, 32, quarter), f32),
        pltpu.VMEM((3, 2, 32, quarter), f32),
        pltpu.VMEM((4, 2, 32, quarter), f32),
        pltpu.VMEM((12, slots, pair, levels, 16, quarter), members.dtype),
        pltpu.VMEM((12, slots, levels, 16, quarter), f32),
        pltpu.VMEM(field, f32),
        pltpu.VMEM(field, f32),
        pltpu.VMEM(field, f32),
        pltpu.VMEM(one, f32),
        pltpu.VMEM(one, f32),
        pltpu.VMEM((3,) + one[1:], f32),
        pltpu.VMEM(one, f32),
        pltpu.VMEM((64, lon), f32),
        pltpu.VMEM((half, 8, lon), f32),
        pltpu.VMEM((half, 8, lon), f32),
        pltpu.VMEM((half, 8, lon), f32),
        pltpu.VMEM((half, 8, lon), f32),
        pltpu.VMEM((64, lon), f32),
        pltpu.VMEM((80, lon), f32),
        dma,
        dma((3,)),
        dma((3,)),
        dma((3,)),
        dma((3,)),
        dma((12, 2)),
        dma,
        dma((10 + 4 * (half - 1),)),
        dma((10 + 4 * (half - 1),)),
        dma((3, 3)),
        dma((3, 3)),
        dma((half + 1, 3)),
        dma((half + 1, 3)),
        dma((half + 1, 3)),
        dma((half + 1, 3)),
        dma((4,)),
        dma((4,)),
    ]
    hbm = pl.BlockSpec(memory_space=pltpu.HBM)
    return pl.pallas_call(
        functools.partial(
            kernel, n_state=sizes["state"], scale=float(n_members - 1) ** -0.5, n_members=n_members
        ),
        out_shape=pltpu.VMEM((half, pair, rows, lon), f32),
        in_specs=[hbm] * 4,
        out_specs=pl.BlockSpec(memory_space=pltpu.VMEM),
        scratch_shapes=scratch,
        compiler_params=pltpu.CompilerParams(
            collective_id=0, has_side_effects=True, vmem_limit_bytes=VMEM_LIMIT
        ),
    )(members, slot_grad, diffusivity, vertical)


VMEM_LIMIT = 50 * 1024 * 1024


def solution(mesh):
    in_specs = (
        P("tm", "member", None, "state", None),
        P("tm", None, "state", None),
        P("state", None),
        P(),
    )
    out_specs = P("tm", "member", "state", None)
    step = functools.partial(body, sizes=dict(mesh.shape))
    return jax.shard_map(step, mesh=mesh, in_specs=in_specs, out_specs=out_specs, check_vma=False)
```

```python
import functools

import jax
import jax.numpy as jnp
from jax import lax
from jax.experimental import pallas as pl
from jax.experimental.pallas import tpu as pltpu
from jax.sharding import PartitionSpec as P

NSTEP = 4
MESH = pl.DeviceIdType.MESH
LANES = 128


def kernel(
    members, slot_grad, diffusivity, matrix, out,
    vertical, pp, pr, pg, mv, gv, cs, co, zr, rb, ps, rsr, sg, kp, hst, hsb, hrt, hrb, w, v,
    v_sem, pre_rs_s, pre_rs_r, pre_ag_s, pre_ag_r, ld_sem, kp_sem, z_s, z_r, ref_s, ref_r, rs_s, rs_r, ag_s, ag_r, h_s, h_r,
    *, n_state, scale, n_members,
):
    f32 = jnp.float32
    tm, mb, st = lax.axis_index("tm"), lax.axis_index("member"), lax.axis_index("state")
    levels = mv.shape[3]
    half = levels // 2
    post = half - 2
    mid = pl.ds(8, 32)
    quarter = mv.shape[-1]
    tiles = quarter // LANES
    zpeer = (1 - tm, mb, st)
    up, down = (tm, mb, st - 1), (tm, mb, st + 1)
    has_up, has_down = st > 0, st < n_state - 1

    def turn(i):
        return lax.rem(mb + i, 4)

    def ypeer(i):
        return (tm, turn(i), st)

    def remote(src, dst, send, recv, peer):
        return pltpu.make_async_remote_copy(
            src_ref=src, dst_ref=dst, send_sem=send, recv_sem=recv, device_id=peer, device_id_type=MESH
        )

    block_rows = (0, 32, 16)

    def loads(s, i):
        rows = pl.ds(block_rows[s], 16)
        lanes = pl.ds(pl.multiple_of(turn(i) * quarter, LANES), quarter)
        j = 4 * s + i
        return (
            pltpu.make_async_copy(members.at[:, :, :, rows, lanes], mv.at[j], ld_sem.at[j, 0]),
            pltpu.make_async_copy(slot_grad.at[:, :, rows, lanes], gv.at[j], ld_sem.at[j, 1]),
        )

    def start_loads(s, i):
        for copy in loads(s, i):
            copy.start()

    vload = pltpu.make_async_copy(matrix, vertical, v_sem)
    vload.start()
    start_loads(0, 0)
    start_loads(1, 0)

    barrier = pltpu.get_barrier_semaphore()
    pl.semaphore_signal(barrier, inc=1, device_id=zpeer, device_id_type=MESH)
    for i in (1, 2, 3):
        pl.semaphore_signal(barrier, inc=1, device_id=ypeer(i), device_id_type=MESH)

    @pl.when(has_up)
    def _():
        pl.semaphore_signal(barrier, inc=1, device_id=up, device_id_type=MESH)

    @pl.when(has_down)
    def _():
        pl.semaphore_signal(barrier, inc=1, device_id=down, device_id_type=MESH)

    kload = pltpu.make_async_copy(diffusivity, kp.at[pl.ds(8, 48)], kp_sem)
    kload.start()
    start_loads(0, 1)

    def z_edge(u, i):
        q, rows = turn(i), pl.ds(40 * u, 8)
        ks = pl.ds(0, 1 if u == 1 and isinstance(i, int) and i == 0 else 2)
        n = 4 * u + i
        return remote(cs.at[q, :, ks, rows], zr.at[q, :, ks, rows], z_s.at[n], z_r.at[n], zpeer)

    def z_mid(l, i):
        q, n = turn(i), 8 + 4 * l + i
        ks = pl.ds(0, 1) if i == 0 else pl.ds(0, 2)
        return remote(cs.at[q, l, ks, mid], zr.at[q, l, ks, mid], z_s.at[n], z_r.at[n], zpeer)

    def z_last(n):
        at = 8 + 4 * post + n
        l, k = post + n // 2, n % 2
        return remote(cs.at[:, l, k, mid], zr.at[:, l, k, mid], z_s.at[at], z_r.at[at], zpeer)

    ref_part = ((pl.ds(0, post), pl.ds(8, 8)), (pl.ds(0, half), pl.ds(32, 16)), (pl.ds(0, post), pl.ds(16, 16)))

    def ref_copy(s, i):
        lv, rows = ref_part[s]
        return remote(
            cs.at[mb, lv, 1, rows], rb.at[mb, lv, rows], ref_s.at[s, i - 1], ref_r.at[s, i - 1], ypeer(4 - i)
        )

    def ref_arrival(s, i):
        lv, rows = ref_part[s]
        here = rb.at[turn(i), lv, rows]
        return remote(here, here, ref_s.at[s, i - 1], ref_r.at[s, i - 1], zpeer)

    def span(u):
        if isinstance(u, int) and u < 2:
            return pl.ds(0, half), pl.ds(40 * u, 8)
        return pl.ds(u - 2, 1), mid

    def rs_copy(u, i):
        lv, rows = span(u)
        q = turn(i)
        return remote(ps.at[q, lv, rows], rsr.at[i - 1, lv, rows], rs_s.at[u, i - 1], rs_r.at[u, i - 1], ypeer(i))

    def ag_copy(u, i):
        lv, rows = span(u)
        here = sg.at[mb, lv, rows]
        return remote(here, here, ag_s.at[u, i - 1], ag_r.at[u, i - 1], ypeer(i))

    def pre_rs(i):
        return remote(pp.at[turn(i)], pr.at[i - 1], pre_rs_s.at[i - 1], pre_rs_r.at[i - 1], ypeer(i))

    def pre_ag(i):
        return remote(pg.at[mb], pg.at[mb], pre_ag_s.at[i - 1], pre_ag_r.at[i - 1], ypeer(i))

    def k_up():
        return remote(kp.at[pl.ds(8, 8)], kp.at[pl.ds(56, 8)], h_s.at[0], h_r.at[0], up)

    def k_down():
        return remote(kp.at[pl.ds(48, 8)], kp.at[pl.ds(0, 8)], h_s.at[1], h_r.at[1], down)

    def f_up():
        return remote(hst, hrb, h_s.at[2], h_r.at[2], up)

    def f_down():
        return remote(hsb, hrt, h_s.at[3], h_r.at[3], down)

    def products(s, i):
        j, q = 4 * s + i, turn(i)
        rows = pl.ds(block_rows[s], 16)
        own = half * tm
        other = half - own

        def tile(n, c):
            k = lax.rem(n, 2)
            lanes = pl.ds(pl.multiple_of((n // 2) * LANES, LANES), LANES)
            part = [
                mv[j, 0, k, m, :, lanes].astype(f32) * gv[j, 0, m, :, lanes]
                + mv[j, 1, k, m, :, lanes].astype(f32) * gv[j, 1, m, :, lanes]
                for m in range(levels)
            ]
            for start, dst in ((other, cs), (own, co)):
                for l in range(half):
                    total = vertical[0, start + l] * part[0]
                    for m in range(1, levels):
                        total = total + vertical[m, start + l] * part[m]
                    dst[q, l, k, rows, lanes] = total
            return c

        lax.fori_loop(0, 2 * tiles, tile, 0)

    ref_tiles = (((8, post),), ((32, post), (40, half)), ((16, post), (24, post)))

    def subtract(s, q, refer, ks):
        for r, count in ref_tiles[s]:
            rows = pl.ds(r, 8)

            def sub(l, c):
                ref = refer(l, rows)
                for k in ks:
                    cs[q, l, k, rows] = cs[q, l, k, rows] - ref
                return c

            lax.fori_loop(0, count, sub, 0)

    def mix(s, i):
        for copy in loads(s, i):
            copy.wait()
        products(s, i)
        if isinstance(i, int) and i == 0:
            if s == 0:
                peers = 4 + has_up.astype(jnp.int32) + has_down.astype(jnp.int32)
                pl.semaphore_wait(barrier, peers)
            for n in (1, 2, 3):
                ref_copy(s, n).start()
            if s == 0:
                z_edge(0, i).start()
            subtract(s, mb, lambda l, rows: cs[mb, l, 1, rows], (0,))
        elif s == 0:
            z_edge(0, i).start()

    def mix_rest(s, after):
        def step(i, c):
            after(i)
            mix(s, i)
            return c

        lax.fori_loop(1, 4, step, 0)

    def refer(s):
        def step(i, c):
            q = turn(i)
            ref_arrival(s, i).wait_recv()
            subtract(s, q, lambda l, rows: rb[q, l, rows], (0, 1))
            if s == 1:
                z_edge(1, i).start()
            return c

        lax.fori_loop(1, 4, step, 0)

    vload.wait()
    start_loads(0, 2)
    mix(0, 0)
    start_loads(0, 3)
    mix(1, 0)
    mix_rest(0, lambda i: start_loads(1, i))
    z_edge(1, 0).start()
    mix_rest(1, lambda i: start_loads(2, i - 1))
    refer(1)
    start_loads(2, 3)
    mix(2, 0)
    mix_rest(2, lambda i: None)
    refer(0)
    refer(2)

    kload.wait()

    @pl.when(has_up)
    def _():
        k_up().start()

    @pl.when(has_down)
    def _():
        k_down().start()

    @pl.when(jnp.logical_not(has_up))
    def _():
        kp[pl.ds(0, 8)] = jnp.zeros((8, kp.shape[1]), f32)
        hrt[...] = jnp.zeros(hrt.shape, f32)

    @pl.when(jnp.logical_not(has_down))
    def _():
        kp[pl.ds(56, 8)] = jnp.zeros((8, kp.shape[1]), f32)
        hrb[...] = jnp.zeros(hrb.shape, f32)

    def add_up(q, l, rows):
        a = co[q, l, 0, rows] + zr[q, l, 0, rows]
        b = co[q, l, 1, rows] + zr[q, l, 1, rows]
        co[q, l, 0, rows] = a
        co[q, l, 1, rows] = b
        ps[q, l, rows] = a + b

    def arrive_edge(u, i):
        z_edge(u, i).wait_recv()
        q = turn(i)

        def body(l, c):
            add_up(q, l, pl.ds(40 * u, 8))
            return c

        lax.fori_loop(0, half, body, 0)
        if i:
            rs_copy(u, i).start()

    def arrive_mid(l):
        for i in range(4):
            z_mid(l, i).wait_recv()
            add_up(turn(i), l, mid)
            if i:
                rs_copy(2 + l, i).start()

    def total(u):
        lv, rows = span(u)
        for i in (1, 2, 3):
            rs_copy(u, i).wait_recv()

        def body(l, c):
            sg[mb, l, rows] = (ps[mb, l, rows] + rsr[0, l, rows]) + (rsr[1, l, rows] + rsr[2, l, rows])
            return c

        lax.fori_loop(lv.start, lv.start + lv.size, body, 0)
        for i in (1, 2, 3):
            ag_copy(u, i).start()

    def centred(u):
        lv, rows = span(u)
        for i in (1, 2, 3):
            q = turn(i)
            pltpu.make_async_remote_copy(
                src_ref=sg.at[q, lv, rows], dst_ref=sg.at[q, lv, rows],
                send_sem=ag_s.at[u, 3 - i], recv_sem=ag_r.at[u, 3 - i],
                device_id=zpeer, device_id_type=MESH,
            ).wait_recv()

        def body(l, c):
            for q in range(4):
                mean = sg[q, l, rows] * (1.0 / n_members)
                for k in range(2):
                    out[l, k, rows, pl.ds(q * quarter, quarter)] = (co[q, l, k, rows] - mean) * scale
            return c

        lax.fori_loop(lv.start, lv.start + lv.size, body, 0)

    def pre_sum():
        for n in range(4):
            q = turn(n)

            def add(l, c):
                for h, src in enumerate((cs, co)):
                    pp[q, h, l] = src[q, post + l, 0, mid] + src[q, post + l, 1, mid]
                return c

            lax.fori_loop(0, 2, add, 0)
            if n:
                pre_rs(n).start()

    def pre_total():
        for i in (1, 2, 3):
            pre_rs(i).wait_recv()

        def add(l, c):
            for h in range(2):
                pg[mb, h, l] = (pp[mb, h, l] + pr[0, h, l]) + (pr[1, h, l] + pr[2, h, l])
            return c

        lax.fori_loop(0, 2, add, 0)
        for i in (1, 2, 3):
            pre_ag(i).start()

    def pre_centred():
        for i in (1, 2, 3):
            here = pg.at[turn(i)]
            remote(here, here, pre_ag_s.at[3 - i], pre_ag_r.at[3 - i], zpeer).wait_recv()
            ref_copy(1, i).wait_send()

        def centre(q, c):
            for l in range(2):
                for h, dst in enumerate((cs, co)):
                    mean = pg[q, h, l] * (1.0 / n_members)
                    for k in range(2):
                        dst[q, post + l, k, mid] = dst[q, post + l, k, mid] - mean
            return c

        lax.fori_loop(0, 4, centre, 0)

    def arrive_last(n):
        z_last(n).wait_recv()
        l, k = post + n // 2, n % 2
        for q in range(4):
            out[l, k, mid, pl.ds(q * quarter, quarter)] = (co[q, l, k, mid] + zr[q, l, k, mid]) * scale

    def edge_top():
        def body(l, c):
            for k in range(2):
                hst[l, pl.ds(4 * k, 4)] = out[l, k, pl.ds(0, 4)]
            return c

        @pl.when(has_up)
        def _():
            lax.fori_loop(0, half, body, 0)
            f_up().start()

    def edge_bottom():
        def body(l, c):
            for k in range(2):
                hsb[l, pl.ds(4 * k, 4)] = out[l, k, pl.ds(44, 4)]
            return c

        @pl.when(has_down)
        def _():
            lax.fori_loop(0, half, body, 0)
            f_down().start()

    def smooth(l, ks=(0, 1)):
        for k in ks:
            w[pl.ds(8, 48)] = out[l, k]
            w[pl.ds(4, 4)] = hrt[l, pl.ds(4 * k, 4)]
            w[pl.ds(56, 4)] = hrb[l, pl.ds(4 * k, 4)]

            row = lax.broadcasted_iota(jnp.int32, (8, w.shape[1]), 0)
            top_row, bottom_row = row == 0, row == 7

            def filter_step(n, c):
                def product(t):
                    v[pl.ds(8 * t + 8, 8)] = kp[pl.ds(8 * t, 8)] * w[pl.ds(8 * t, 8)]

                product(0)
                for t in range(8):
                    if t < 7:
                        product(t + 1)
                    before, at, after = (v[pl.ds(8 * t + 8 * n, 8)] for n in range(3))
                    around = pltpu.roll(at, 1, 1) + pltpu.roll(at, at.shape[1] - 1, 1)
                    around = around + pltpu.roll(jnp.where(bottom_row, before, at), 1, 0)
                    around = around + pltpu.roll(jnp.where(top_row, after, at), 7, 0)
                    w[pl.ds(8 * t, 8)] = (w[pl.ds(8 * t, 8)] - 4.0 * at) + around
                return c

            lax.fori_loop(0, NSTEP, filter_step, 0)
            out[l, k] = w[pl.ds(8, 48)]

    def wait_halos():
        @pl.when(has_up)
        def _():
            k_down().wait_recv()
            f_down().wait_recv()

        @pl.when(has_down)
        def _():
            k_up().wait_recv()
            f_up().wait_recv()

    w[pl.ds(0, 8)] = jnp.zeros((8, w.shape[1]), f32)
    w[pl.ds(56, 8)] = jnp.zeros((8, w.shape[1]), f32)
    zr[mb, pl.ds(0, post), 1, pl.ds(8, 40)] = jnp.zeros((post, 40, quarter), f32)
    zr[mb, pl.ds(post, 2), 1, pl.ds(40, 8)] = jnp.zeros((2, 8, quarter), f32)
    v[pl.ds(0, 8)] = jnp.zeros((8, v.shape[1]), f32)
    v[pl.ds(72, 8)] = jnp.zeros((8, v.shape[1]), f32)

    def start_mid(l):
        for i in range(4):
            z_mid(l, i).start()

    start_mid(0)
    start_mid(1)
    for i in range(4):
        arrive_edge(0, i)
    arrive_edge(1, 0)
    arrive_edge(1, 1)
    total(0)
    start_mid(2)
    arrive_edge(1, 2)
    arrive_edge(1, 3)
    start_mid(3)
    total(1)
    centred(0)
    edge_top()
    pre_sum()
    start_mid(4)
    start_mid(5)
    arrive_mid(0)
    centred(1)
    edge_bottom()
    arrive_mid(1)
    total(2)
    pre_total()
    arrive_mid(2)
    total(3)
    wait_halos()
    centred(2)
    smooth(0)
    pre_centred()
    for n in range(4):
        z_last(n).start()

    def rest(l, c):
        arrive_mid(l)
        total(l + 1)
        centred(l)
        smooth(l - 2)
        return c

    lax.fori_loop(3, post, rest, 0)
    total(post + 1)
    centred(post)
    smooth(post - 2)
    arrive_last(0)
    smooth(post, (0,))
    centred(post + 1)
    smooth(post - 1)
    arrive_last(1)
    smooth(post, (1,))
    for k in range(2):
        arrive_last(2 + k)
        smooth(post + 1, (k,))

    for u in range(2):
        for i in range(4):
            z_edge(u, i).wait_send()
    for n in range(4):
        z_last(n).wait_send()

    def sent(l, c):
        for i in range(4):
            z_mid(l, i).wait_send()
        return c

    lax.fori_loop(0, post, sent, 0)
    for i in (1, 2, 3):
        pre_rs(i).wait_send()
        pre_ag(i).wait_send()
        for s in (0, 2):
            ref_copy(s, i).wait_send()
        for u in (0, 1):
            rs_copy(u, i).wait_send()
            ag_copy(u, i).wait_send()

    def sums_sent(u, c):
        for i in (1, 2, 3):
            rs_copy(u, i).wait_send()
            ag_copy(u, i).wait_send()
        return c

    lax.fori_loop(2, post + 2, sums_sent, 0)

    @pl.when(has_up)
    def _():
        k_up().wait_send()
        f_up().wait_send()

    @pl.when(has_down)
    def _():
        k_down().wait_send()
        f_down().wait_send()


def body(members, slot_grad, diffusivity, vertical, *, sizes):
    slots, pair, levels, rows, lon = members.shape
    half, quarter = levels // sizes["tm"], lon // 4
    n_members = pair * sizes["member"]
    dma = pltpu.SemaphoreType.DMA
    f32 = jnp.float32
    field = (4, half, pair, rows, quarter)
    one = (4, half, rows, quarter)
    scratch = [
        pltpu.SMEM((levels, levels), f32),
        pltpu.VMEM((4, 2, 2, 32, quarter), f32),
        pltpu.VMEM((3, 2, 2, 32, quarter), f32),
        pltpu.VMEM((4, 2, 2, 32, quarter), f32),
        pltpu.VMEM((12, slots, pair, levels, 16, quarter), members.dtype),
        pltpu.VMEM((12, slots, levels, 16, quarter), f32),
        pltpu.VMEM(field, f32),
        pltpu.VMEM(field, f32),
        pltpu.VMEM(field, f32),
        pltpu.VMEM(one, f32),
        pltpu.VMEM(one, f32),
        pltpu.VMEM((3,) + one[1:], f32),
        pltpu.VMEM(one, f32),
        pltpu.VMEM((64, lon), f32),
        pltpu.VMEM((half, 8, lon), f32),
        pltpu.VMEM((half, 8, lon), f32),
        pltpu.VMEM((half, 8, lon), f32),
        pltpu.VMEM((half, 8, lon), f32),
        pltpu.VMEM((64, lon), f32),
        pltpu.VMEM((80, lon), f32),
        dma,
        dma((3,)),
        dma((3,)),
        dma((3,)),
        dma((3,)),
        dma((12, 2)),
        dma,
        dma((12 + 4 * (half - 2),)),
        dma((12 + 4 * (half - 2),)),
        dma((3, 3)),
        dma((3, 3)),
        dma((half, 3)),
        dma((half, 3)),
        dma((half, 3)),
        dma((half, 3)),
        dma((4,)),
        dma((4,)),
    ]
    hbm = pl.BlockSpec(memory_space=pltpu.HBM)
    return pl.pallas_call(
        functools.partial(
            kernel, n_state=sizes["state"], scale=float(n_members - 1) ** -0.5, n_members=n_members
        ),
        out_shape=pltpu.VMEM((half, pair, rows, lon), f32),
        in_specs=[hbm] * 4,
        out_specs=pl.BlockSpec(memory_space=pltpu.VMEM),
        scratch_shapes=scratch,
        compiler_params=pltpu.CompilerParams(
            collective_id=0, has_side_effects=True, vmem_limit_bytes=VMEM_LIMIT
        ),
    )(members, slot_grad, diffusivity, vertical)


VMEM_LIMIT = 50 * 1024 * 1024


def solution(mesh):
    in_specs = (
        P("tm", "member", None, "state", None),
        P("tm", None, "state", None),
        P("state", None),
        P(),
    )
    out_specs = P("tm", "member", "state", None)
    step = functools.partial(body, sizes=dict(mesh.shape))
    return jax.shard_map(step, mesh=mesh, in_specs=in_specs, out_specs=out_specs, check_vma=False)
```

```python
import functools

import jax
import jax.numpy as jnp
from jax import lax
from jax.experimental import pallas as pl
from jax.experimental.pallas import tpu as pltpu
from jax.sharding import PartitionSpec as P

NSTEP = 4
MESH = pl.DeviceIdType.MESH
LANES = 128


def kernel(
    members, slot_grad, diffusivity, matrix, out,
    vertical, pp, pr, pg, mv, gv, cs, co, zr, rb, ps, rsr, sg, kp, hst, hsb, hrt, hrb, hrelay, w, v,
    v_sem, pre_rs_s, pre_rs_r, pre_ag_s, pre_ag_r, ld_sem, kp_sem, z_s, z_r, ref_s, ref_r, rs_s, rs_r, ag_s, ag_r, h_s, h_r, part_s, part_r, relay_s,
    *, n_state, scale, n_members,
):
    f32 = jnp.float32
    tm, mb, st = lax.axis_index("tm"), lax.axis_index("member"), lax.axis_index("state")
    levels = mv.shape[3]
    half = levels // 2
    post = half - 2
    mid = pl.ds(8, 32)
    quarter = mv.shape[-1]
    tiles = quarter // LANES
    zpeer = (1 - tm, mb, st)
    up, down = (tm, mb, st - 1), (tm, mb, st + 1)
    has_up, has_down = st > 0, st < n_state - 1
    cut = n_state // 2
    parts = half // 2
    over, under = st == cut - 1, st == cut
    at_cut = jnp.logical_or(over, under)
    hop = jnp.where(st < cut, cut - 1 - st, st - cut)
    is_relay = jnp.logical_and(lax.rem(hop, 2) == 0, jnp.logical_and(hop > 0, hop < 2 * parts - 2))
    turn_of = hop // 2

    def lower(p):
        return (tm, mb, cut + 2 * p)

    def upper(p):
        return (tm, mb, cut - 1 - 2 * p)

    def turn(i):
        return lax.rem(mb + i, 4)

    def ypeer(i):
        return (tm, turn(i), st)

    def remote(src, dst, send, recv, peer):
        return pltpu.make_async_remote_copy(
            src_ref=src, dst_ref=dst, send_sem=send, recv_sem=recv, device_id=peer, device_id_type=MESH
        )

    block_rows = (0, 32, 16)

    def loads(s, i):
        rows = pl.ds(block_rows[s], 16)
        lanes = pl.ds(pl.multiple_of(turn(i) * quarter, LANES), quarter)
        j = 4 * s + i
        return (
            pltpu.make_async_copy(members.at[:, :, :, rows, lanes], mv.at[j], ld_sem.at[j, 0]),
            pltpu.make_async_copy(slot_grad.at[:, :, rows, lanes], gv.at[j], ld_sem.at[j, 1]),
        )

    def start_loads(s, i):
        for copy in loads(s, i):
            copy.start()

    vload = pltpu.make_async_copy(matrix, vertical, v_sem)
    vload.start()
    start_loads(0, 0)
    start_loads(1, 0)

    barrier = pltpu.get_barrier_semaphore()
    pl.semaphore_signal(barrier, inc=1, device_id=zpeer, device_id_type=MESH)
    for i in (1, 2, 3):
        pl.semaphore_signal(barrier, inc=1, device_id=ypeer(i), device_id_type=MESH)

    @pl.when(at_cut)
    def _():
        for p in range(1, parts - 1):
            pl.semaphore_signal(barrier, inc=1, device_id=lower(p), device_id_type=MESH)
            pl.semaphore_signal(barrier, inc=1, device_id=upper(p), device_id_type=MESH)

    @pl.when(is_relay)
    def _():
        pl.semaphore_signal(barrier, inc=1, device_id=lower(0), device_id_type=MESH)
        pl.semaphore_signal(barrier, inc=1, device_id=upper(0), device_id_type=MESH)

    @pl.when(has_up)
    def _():
        pl.semaphore_signal(barrier, inc=1, device_id=up, device_id_type=MESH)

    @pl.when(has_down)
    def _():
        pl.semaphore_signal(barrier, inc=1, device_id=down, device_id_type=MESH)

    kload = pltpu.make_async_copy(diffusivity, kp.at[pl.ds(8, 48)], kp_sem)
    kload.start()
    start_loads(0, 1)

    def z_edge(u, i):
        q, rows = turn(i), pl.ds(40 * u, 8)
        ks = pl.ds(0, 1 if u == 1 and isinstance(i, int) and i == 0 else 2)
        n = 4 * u + i
        return remote(cs.at[q, :, ks, rows], zr.at[q, :, ks, rows], z_s.at[n], z_r.at[n], zpeer)

    def z_mid(l, i):
        q, n = turn(i), 8 + 4 * l + i
        ks = pl.ds(0, 1) if i == 0 else pl.ds(0, 2)
        return remote(cs.at[q, l, ks, mid], zr.at[q, l, ks, mid], z_s.at[n], z_r.at[n], zpeer)

    def z_last(n):
        at = 8 + 4 * post + n
        l, k = post + n // 2, n % 2
        return remote(cs.at[:, l, k, mid], zr.at[:, l, k, mid], z_s.at[at], z_r.at[at], zpeer)

    ref_part = ((pl.ds(0, post), pl.ds(8, 8)), (pl.ds(0, half), pl.ds(32, 16)), (pl.ds(0, post), pl.ds(16, 16)))

    def ref_copy(s, i):
        lv, rows = ref_part[s]
        return remote(
            cs.at[mb, lv, 1, rows], rb.at[mb, lv, rows], ref_s.at[s, i - 1], ref_r.at[s, i - 1], ypeer(4 - i)
        )

    def ref_arrival(s, i):
        lv, rows = ref_part[s]
        here = rb.at[turn(i), lv, rows]
        return remote(here, here, ref_s.at[s, i - 1], ref_r.at[s, i - 1], zpeer)

    def span(u):
        if isinstance(u, int) and u < 2:
            return pl.ds(0, half), pl.ds(40 * u, 8)
        return pl.ds(u - 2, 1), mid

    def rs_copy(u, i):
        lv, rows = span(u)
        q = turn(i)
        return remote(ps.at[q, lv, rows], rsr.at[i - 1, lv, rows], rs_s.at[u, i - 1], rs_r.at[u, i - 1], ypeer(i))

    def ag_copy(u, i):
        lv, rows = span(u)
        here = sg.at[mb, lv, rows]
        return remote(here, here, ag_s.at[u, i - 1], ag_r.at[u, i - 1], ypeer(i))

    def pre_rs(i):
        return remote(pp.at[turn(i)], pr.at[i - 1], pre_rs_s.at[i - 1], pre_rs_r.at[i - 1], ypeer(i))

    def pre_ag(i):
        return remote(pg.at[mb], pg.at[mb], pre_ag_s.at[i - 1], pre_ag_r.at[i - 1], ypeer(i))

    def k_up():
        return remote(kp.at[pl.ds(8, 8)], kp.at[pl.ds(56, 8)], h_s.at[0], h_r.at[0], up)

    def k_down():
        return remote(kp.at[pl.ds(48, 8)], kp.at[pl.ds(0, 8)], h_s.at[1], h_r.at[1], down)

    def f_up():
        return remote(hst, hrb, h_s.at[2], h_r.at[2], up)

    def f_down():
        return remote(hsb, hrt, h_s.at[3], h_r.at[3], down)

    def f_up_part(p):
        lv = pl.ds(2 * p, 2)
        if p == 0:
            return remote(hst.at[lv], hrb.at[lv], h_s.at[2], h_r.at[2], up)
        if p == parts - 1:
            return remote(hst.at[lv], hrb.at[lv], part_s.at[p - 1], part_r.at[p - 1], up)
        return remote(hst.at[lv], hrelay, part_s.at[p - 1], part_r.at[3], upper(p))

    def f_down_part(p):
        lv = pl.ds(2 * p, 2)
        if p == 0:
            return remote(hsb.at[lv], hrt.at[lv], h_s.at[3], h_r.at[3], down)
        if p == parts - 1:
            return remote(hsb.at[lv], hrt.at[lv], part_s.at[p - 1], part_r.at[p - 1], down)
        return remote(hsb.at[lv], hrelay, part_s.at[p - 1], part_r.at[3], lower(p))

    def relay_up():
        dst = hrb.at[pl.ds(2 * turn_of, 2)]
        return remote(hrelay, dst, relay_s, part_r.at[turn_of - 1], upper(0))

    def relay_down():
        dst = hrt.at[pl.ds(2 * turn_of, 2)]
        return remote(hrelay, dst, relay_s, part_r.at[turn_of - 1], lower(0))

    def part_arrival(dst, p):
        here = dst.at[pl.ds(2 * p, 2)]
        return remote(here, here, part_s.at[p - 1], part_r.at[p - 1], zpeer)

    def pass_on():
        @pl.when(is_relay)
        def _():
            remote(hrelay, hrelay, relay_s, part_r.at[3], zpeer).wait_recv()

            @pl.when(st < cut)
            def _():
                relay_up().start()

            @pl.when(st > cut)
            def _():
                relay_down().start()

    def parts_arrive():
        @pl.when(over)
        def _():
            for p in range(1, parts):
                part_arrival(hrb, p).wait_recv()

        @pl.when(under)
        def _():
            for p in range(1, parts):
                part_arrival(hrt, p).wait_recv()

    def products(s, i):
        j, q = 4 * s + i, turn(i)
        rows = pl.ds(block_rows[s], 16)
        own = half * tm
        other = half - own

        def tile(n, c):
            k = lax.rem(n, 2)
            lanes = pl.ds(pl.multiple_of((n // 2) * LANES, LANES), LANES)
            part = [
                mv[j, 0, k, m, :, lanes].astype(f32) * gv[j, 0, m, :, lanes]
                + mv[j, 1, k, m, :, lanes].astype(f32) * gv[j, 1, m, :, lanes]
                for m in range(levels)
            ]
            for start, dst in ((other, cs), (own, co)):
                for l in range(half):
                    total = vertical[0, start + l] * part[0]
                    for m in range(1, levels):
                        total = total + vertical[m, start + l] * part[m]
                    dst[q, l, k, rows, lanes] = total
            return c

        lax.fori_loop(0, 2 * tiles, tile, 0)

    ref_tiles = (((8, post),), ((32, post), (40, half)), ((16, post), (24, post)))

    def subtract(s, q, refer, ks):
        for r, count in ref_tiles[s]:
            rows = pl.ds(r, 8)

            def sub(l, c):
                ref = refer(l, rows)
                for k in ks:
                    cs[q, l, k, rows] = cs[q, l, k, rows] - ref
                return c

            lax.fori_loop(0, count, sub, 0)

    def mix(s, i):
        for copy in loads(s, i):
            copy.wait()
        products(s, i)
        if isinstance(i, int) and i == 0:
            if s == 0:
                peers = 4 + has_up.astype(jnp.int32) + has_down.astype(jnp.int32)
                peers = peers + 2 * (parts - 2) * at_cut.astype(jnp.int32) + 2 * is_relay.astype(jnp.int32)
                pl.semaphore_wait(barrier, peers)
            for n in (1, 2, 3):
                ref_copy(s, n).start()
            if s == 0:
                z_edge(0, i).start()
            subtract(s, mb, lambda l, rows: cs[mb, l, 1, rows], (0,))
        elif s == 0:
            z_edge(0, i).start()

    def mix_rest(s, after):
        def step(i, c):
            after(i)
            mix(s, i)
            return c

        lax.fori_loop(1, 4, step, 0)

    def refer(s):
        def step(i, c):
            q = turn(i)
            ref_arrival(s, i).wait_recv()
            subtract(s, q, lambda l, rows: rb[q, l, rows], (0, 1))
            if s == 1:
                z_edge(1, i).start()
            return c

        lax.fori_loop(1, 4, step, 0)

    vload.wait()
    start_loads(0, 2)
    mix(0, 0)
    start_loads(0, 3)
    mix(1, 0)
    mix_rest(0, lambda i: start_loads(1, i))
    z_edge(1, 0).start()
    mix_rest(1, lambda i: start_loads(2, i - 1))
    refer(1)
    start_loads(2, 3)
    mix(2, 0)
    mix_rest(2, lambda i: None)
    refer(0)
    refer(2)

    kload.wait()

    @pl.when(has_up)
    def _():
        k_up().start()

    @pl.when(has_down)
    def _():
        k_down().start()

    @pl.when(jnp.logical_not(has_up))
    def _():
        kp[pl.ds(0, 8)] = jnp.zeros((8, kp.shape[1]), f32)
        hrt[...] = jnp.zeros(hrt.shape, f32)

    @pl.when(jnp.logical_not(has_down))
    def _():
        kp[pl.ds(56, 8)] = jnp.zeros((8, kp.shape[1]), f32)
        hrb[...] = jnp.zeros(hrb.shape, f32)

    def add_up(q, l, rows):
        a = co[q, l, 0, rows] + zr[q, l, 0, rows]
        b = co[q, l, 1, rows] + zr[q, l, 1, rows]
        co[q, l, 0, rows] = a
        co[q, l, 1, rows] = b
        ps[q, l, rows] = a + b

    def arrive_edge(u, i):
        z_edge(u, i).wait_recv()
        q = turn(i)

        def body(l, c):
            add_up(q, l, pl.ds(40 * u, 8))
            return c

        lax.fori_loop(0, half, body, 0)
        if i:
            rs_copy(u, i).start()

    def arrive_mid(l):
        for i in range(4):
            z_mid(l, i).wait_recv()
            add_up(turn(i), l, mid)
            if i:
                rs_copy(2 + l, i).start()

    def total(u):
        lv, rows = span(u)
        for i in (1, 2, 3):
            rs_copy(u, i).wait_recv()

        def body(l, c):
            sg[mb, l, rows] = (ps[mb, l, rows] + rsr[0, l, rows]) + (rsr[1, l, rows] + rsr[2, l, rows])
            return c

        lax.fori_loop(lv.start, lv.start + lv.size, body, 0)
        for i in (1, 2, 3):
            ag_copy(u, i).start()

    def centred(u):
        lv, rows = span(u)
        for i in (1, 2, 3):
            q = turn(i)
            pltpu.make_async_remote_copy(
                src_ref=sg.at[q, lv, rows], dst_ref=sg.at[q, lv, rows],
                send_sem=ag_s.at[u, 3 - i], recv_sem=ag_r.at[u, 3 - i],
                device_id=zpeer, device_id_type=MESH,
            ).wait_recv()

        def body(l, c):
            for q in range(4):
                mean = sg[q, l, rows] * (1.0 / n_members)
                for k in range(2):
                    out[l, k, rows, pl.ds(q * quarter, quarter)] = (co[q, l, k, rows] - mean) * scale
            return c

        lax.fori_loop(lv.start, lv.start + lv.size, body, 0)

    def pre_sum():
        for n in range(4):
            q = turn(n)

            def add(l, c):
                for h, src in enumerate((cs, co)):
                    pp[q, h, l] = src[q, post + l, 0, mid] + src[q, post + l, 1, mid]
                return c

            lax.fori_loop(0, 2, add, 0)
            if n:
                pre_rs(n).start()

    def pre_total():
        for i in (1, 2, 3):
            pre_rs(i).wait_recv()

        def add(l, c):
            for h in range(2):
                pg[mb, h, l] = (pp[mb, h, l] + pr[0, h, l]) + (pr[1, h, l] + pr[2, h, l])
            return c

        lax.fori_loop(0, 2, add, 0)
        for i in (1, 2, 3):
            pre_ag(i).start()

    def pre_centred():
        for i in (1, 2, 3):
            here = pg.at[turn(i)]
            remote(here, here, pre_ag_s.at[3 - i], pre_ag_r.at[3 - i], zpeer).wait_recv()
            ref_copy(1, i).wait_send()

        def centre(q, c):
            for l in range(2):
                for h, dst in enumerate((cs, co)):
                    mean = pg[q, h, l] * (1.0 / n_members)
                    for k in range(2):
                        dst[q, post + l, k, mid] = dst[q, post + l, k, mid] - mean
            return c

        lax.fori_loop(0, 4, centre, 0)

    def arrive_last(n):
        z_last(n).wait_recv()
        l, k = post + n // 2, n % 2
        for q in range(4):
            out[l, k, mid, pl.ds(q * quarter, quarter)] = (co[q, l, k, mid] + zr[q, l, k, mid]) * scale

    def edge_top():
        def body(l, c):
            for k in range(2):
                hst[l, pl.ds(4 * k, 4)] = out[l, k, pl.ds(0, 4)]
            return c

        @pl.when(has_up)
        def _():
            lax.fori_loop(0, half, body, 0)

            @pl.when(under)
            def _():
                for p in range(parts):
                    f_up_part(p).start()

            @pl.when(jnp.logical_not(under))
            def _():
                f_up().start()

    def edge_bottom():
        def body(l, c):
            for k in range(2):
                hsb[l, pl.ds(4 * k, 4)] = out[l, k, pl.ds(44, 4)]
            return c

        @pl.when(has_down)
        def _():
            lax.fori_loop(0, half, body, 0)

            @pl.when(over)
            def _():
                for p in range(parts):
                    f_down_part(p).start()

            @pl.when(jnp.logical_not(over))
            def _():
                f_down().start()

    def smooth(l, ks=(0, 1)):
        for k in ks:
            w[pl.ds(8, 48)] = out[l, k]
            w[pl.ds(4, 4)] = hrt[l, pl.ds(4 * k, 4)]
            w[pl.ds(56, 4)] = hrb[l, pl.ds(4 * k, 4)]

            row = lax.broadcasted_iota(jnp.int32, (8, w.shape[1]), 0)
            top_row, bottom_row = row == 0, row == 7

            def filter_step(n, c):
                def product(t):
                    v[pl.ds(8 * t + 8, 8)] = kp[pl.ds(8 * t, 8)] * w[pl.ds(8 * t, 8)]

                product(0)
                for t in range(8):
                    if t < 7:
                        product(t + 1)
                    before, at, after = (v[pl.ds(8 * t + 8 * n, 8)] for n in range(3))
                    around = pltpu.roll(at, 1, 1) + pltpu.roll(at, at.shape[1] - 1, 1)
                    around = around + pltpu.roll(jnp.where(bottom_row, before, at), 1, 0)
                    around = around + pltpu.roll(jnp.where(top_row, after, at), 7, 0)
                    w[pl.ds(8 * t, 8)] = (w[pl.ds(8 * t, 8)] - 4.0 * at) + around
                return c

            lax.fori_loop(0, NSTEP, filter_step, 0)
            out[l, k] = w[pl.ds(8, 48)]

    def wait_halos():
        @pl.when(has_up)
        def _():
            k_down().wait_recv()

            @pl.when(under)
            def _():
                f_down_part(0).wait_recv()

            @pl.when(jnp.logical_not(under))
            def _():
                f_down().wait_recv()

        @pl.when(has_down)
        def _():
            k_up().wait_recv()

            @pl.when(over)
            def _():
                f_up_part(0).wait_recv()

            @pl.when(jnp.logical_not(over))
            def _():
                f_up().wait_recv()

    w[pl.ds(0, 8)] = jnp.zeros((8, w.shape[1]), f32)
    w[pl.ds(56, 8)] = jnp.zeros((8, w.shape[1]), f32)
    zr[mb, pl.ds(0, post), 1, pl.ds(8, 40)] = jnp.zeros((post, 40, quarter), f32)
    zr[mb, pl.ds(post, 2), 1, pl.ds(40, 8)] = jnp.zeros((2, 8, quarter), f32)
    v[pl.ds(0, 8)] = jnp.zeros((8, v.shape[1]), f32)
    v[pl.ds(72, 8)] = jnp.zeros((8, v.shape[1]), f32)

    def mid_sent(l):
        for i in range(4):
            z_mid(l, i).wait_send()

    def sums_sent(u):
        for i in (1, 2, 3):
            rs_copy(u, i).wait_send()
            ag_copy(u, i).wait_send()

    def edges_sent():
        @pl.when(is_relay)
        def _():
            remote(hrelay, hrelay, relay_s, part_r.at[3], zpeer).wait_send()

        for u in range(2):
            for i in range(4):
                z_edge(u, i).wait_send()
            sums_sent(u)
        for i in (1, 2, 3):
            ref_copy(0, i).wait_send()
            ref_copy(2, i).wait_send()

        @pl.when(has_up)
        def _():
            k_up().wait_send()

            @pl.when(under)
            def _():
                for p in range(parts):
                    f_up_part(p).wait_send()

            @pl.when(jnp.logical_not(under))
            def _():
                f_up().wait_send()

        @pl.when(has_down)
        def _():
            k_down().wait_send()

            @pl.when(over)
            def _():
                for p in range(parts):
                    f_down_part(p).wait_send()

            @pl.when(jnp.logical_not(over))
            def _():
                f_down().wait_send()

    def start_mid(l):
        for i in range(4):
            z_mid(l, i).start()

    start_mid(0)
    start_mid(1)
    for i in range(4):
        arrive_edge(0, i)
    arrive_edge(1, 0)
    arrive_edge(1, 1)
    total(0)
    start_mid(2)
    arrive_edge(1, 2)
    arrive_edge(1, 3)
    start_mid(3)
    total(1)
    centred(0)
    edge_top()
    pre_sum()
    start_mid(4)
    start_mid(5)
    arrive_mid(0)
    centred(1)
    edge_bottom()
    arrive_mid(1)
    total(2)
    pass_on()
    pre_total()
    arrive_mid(2)
    total(3)
    wait_halos()
    centred(2)
    smooth(0)
    pre_centred()
    for n in range(4):
        z_last(n).start()
    edges_sent()
    parts_arrive()

    def rest(l, c):
        arrive_mid(l)
        total(l + 1)
        centred(l)
        smooth(l - 2)
        mid_sent(l - 3)
        sums_sent(l - 1)
        return c

    lax.fori_loop(3, post, rest, 0)
    total(post + 1)
    centred(post)
    smooth(post - 2)
    arrive_last(0)
    smooth(post, (0,))
    centred(post + 1)
    smooth(post - 1)
    for n in (post - 3, post - 2, post - 1):
        mid_sent(n)
        sums_sent(n + 2)
    arrive_last(1)
    smooth(post, (1,))
    arrive_last(2)
    smooth(post + 1, (0,))
    for i in (1, 2, 3):
        pre_rs(i).wait_send()
        pre_ag(i).wait_send()
    z_last(0).wait_send()
    z_last(1).wait_send()
    arrive_last(3)
    smooth(post + 1, (1,))

    z_last(2).wait_send()
    z_last(3).wait_send()


def body(members, slot_grad, diffusivity, vertical, *, sizes):
    slots, pair, levels, rows, lon = members.shape
    half, quarter = levels // sizes["tm"], lon // 4
    n_members = pair * sizes["member"]
    dma = pltpu.SemaphoreType.DMA
    f32 = jnp.float32
    field = (4, half, pair, rows, quarter)
    one = (4, half, rows, quarter)
    scratch = [
        pltpu.SMEM((levels, levels), f32),
        pltpu.VMEM((4, 2, 2, 32, quarter), f32),
        pltpu.VMEM((3, 2, 2, 32, quarter), f32),
        pltpu.VMEM((4, 2, 2, 32, quarter), f32),
        pltpu.VMEM((12, slots, pair, levels, 16, quarter), members.dtype),
        pltpu.VMEM((12, slots, levels, 16, quarter), f32),
        pltpu.VMEM(field, f32),
        pltpu.VMEM(field, f32),
        pltpu.VMEM(field, f32),
        pltpu.VMEM(one, f32),
        pltpu.VMEM(one, f32),
        pltpu.VMEM((3,) + one[1:], f32),
        pltpu.VMEM(one, f32),
        pltpu.VMEM((64, lon), f32),
        pltpu.VMEM((half, 8, lon), f32),
        pltpu.VMEM((half, 8, lon), f32),
        pltpu.VMEM((half, 8, lon), f32),
        pltpu.VMEM((half, 8, lon), f32),
        pltpu.VMEM((2, 8, lon), f32),
        pltpu.VMEM((64, lon), f32),
        pltpu.VMEM((80, lon), f32),
        dma,
        dma((3,)),
        dma((3,)),
        dma((3,)),
        dma((3,)),
        dma((12, 2)),
        dma,
        dma((12 + 4 * (half - 2),)),
        dma((12 + 4 * (half - 2),)),
        dma((3, 3)),
        dma((3, 3)),
        dma((half, 3)),
        dma((half, 3)),
        dma((half, 3)),
        dma((half, 3)),
        dma((4,)),
        dma((4,)),
        dma((3,)),
        dma((4,)),
        dma,
    ]
    hbm = pl.BlockSpec(memory_space=pltpu.HBM)
    return pl.pallas_call(
        functools.partial(
            kernel, n_state=sizes["state"], scale=float(n_members - 1) ** -0.5, n_members=n_members
        ),
        out_shape=pltpu.VMEM((half, pair, rows, lon), f32),
        in_specs=[hbm] * 4,
        out_specs=pl.BlockSpec(memory_space=pltpu.VMEM),
        scratch_shapes=scratch,
        compiler_params=pltpu.CompilerParams(
            collective_id=0, has_side_effects=True, vmem_limit_bytes=VMEM_LIMIT
        ),
    )(members, slot_grad, diffusivity, vertical)


VMEM_LIMIT = 50 * 1024 * 1024


def solution(mesh):
    in_specs = (
        P("tm", "member", None, "state", None),
        P("tm", None, "state", None),
        P("state", None),
        P(),
    )
    out_specs = P("tm", "member", "state", None)
    step = functools.partial(body, sizes=dict(mesh.shape))
    return jax.shard_map(step, mesh=mesh, in_specs=in_specs, out_specs=out_specs, check_vma=False)
```

```python
import functools

import jax
import jax.numpy as jnp
from jax import lax
from jax.experimental import pallas as pl
from jax.experimental.pallas import tpu as pltpu
from jax.sharding import PartitionSpec as P

NSTEP = 4
MESH = pl.DeviceIdType.MESH
LANES = 128


def kernel(
    members, slot_grad, diffusivity, matrix, out,
    vertical, pp, pr, pg, mv, gv, cs, co, zr, rb, ps, rsr, sg, kp, hst, hsb, hrt, hrb, hrelay, w, v,
    v_sem, pre_rs_s, pre_rs_r, pre_ag_s, pre_ag_r, ld_sem, kp_sem, z_s, z_r, ref_s, ref_r, rs_s, rs_r, ag_s, ag_r, h_s, h_r, part_s, part_r, relay_s,
    *, n_state, scale, n_members,
):
    f32 = jnp.float32
    tm, mb, st = lax.axis_index("tm"), lax.axis_index("member"), lax.axis_index("state")
    levels = mv.shape[3]
    half = levels // 2
    post = half - 2
    mid = pl.ds(8, 32)
    quarter = mv.shape[-1]
    tiles = quarter // LANES
    zpeer = (1 - tm, mb, st)
    up, down = (tm, mb, st - 1), (tm, mb, st + 1)
    has_up, has_down = st > 0, st < n_state - 1
    cut = n_state // 2
    parts = half // 2
    over, under = st == cut - 1, st == cut
    at_cut = jnp.logical_or(over, under)
    hop = jnp.where(st < cut, cut - 1 - st, st - cut)
    is_relay = jnp.logical_and(lax.rem(hop, 2) == 0, jnp.logical_and(hop > 0, hop < 2 * parts - 2))
    turn_of = hop // 2

    def lower(p):
        return (tm, mb, cut + 2 * p)

    def upper(p):
        return (tm, mb, cut - 1 - 2 * p)

    def turn(i):
        return lax.rem(mb + i, 4)

    def ypeer(i):
        return (tm, turn(i), st)

    def remote(src, dst, send, recv, peer):
        return pltpu.make_async_remote_copy(
            src_ref=src, dst_ref=dst, send_sem=send, recv_sem=recv, device_id=peer, device_id_type=MESH
        )

    block_rows = (0, 32, 16)

    def loads(s, i):
        rows = pl.ds(block_rows[s], 16)
        lanes = pl.ds(pl.multiple_of(turn(i) * quarter, LANES), quarter)
        j = 4 * s + i
        return (
            pltpu.make_async_copy(members.at[:, :, :, rows, lanes], mv.at[j], ld_sem.at[j, 0]),
            pltpu.make_async_copy(slot_grad.at[:, :, rows, lanes], gv.at[j], ld_sem.at[j, 1]),
        )

    def start_loads(s, i):
        for copy in loads(s, i):
            copy.start()

    vload = pltpu.make_async_copy(matrix, vertical, v_sem)
    vload.start()
    start_loads(0, 0)
    start_loads(1, 0)

    barrier = pltpu.get_barrier_semaphore()
    pl.semaphore_signal(barrier, inc=1, device_id=zpeer, device_id_type=MESH)
    for i in (1, 2, 3):
        pl.semaphore_signal(barrier, inc=1, device_id=ypeer(i), device_id_type=MESH)

    @pl.when(at_cut)
    def _():
        for p in range(1, parts - 1):
            pl.semaphore_signal(barrier, inc=1, device_id=lower(p), device_id_type=MESH)
            pl.semaphore_signal(barrier, inc=1, device_id=upper(p), device_id_type=MESH)

    @pl.when(is_relay)
    def _():
        pl.semaphore_signal(barrier, inc=1, device_id=lower(0), device_id_type=MESH)
        pl.semaphore_signal(barrier, inc=1, device_id=upper(0), device_id_type=MESH)

    @pl.when(has_up)
    def _():
        pl.semaphore_signal(barrier, inc=1, device_id=up, device_id_type=MESH)

    @pl.when(has_down)
    def _():
        pl.semaphore_signal(barrier, inc=1, device_id=down, device_id_type=MESH)

    kload = pltpu.make_async_copy(diffusivity, kp.at[pl.ds(8, 48)], kp_sem)
    kload.start()
    start_loads(0, 1)

    def z_edge(u, i):
        q, rows = turn(i), pl.ds(40 * u, 8)
        ks = pl.ds(0, 1 if u == 1 and isinstance(i, int) and i == 0 else 2)
        n = 4 * u + i
        return remote(cs.at[q, :, ks, rows], zr.at[q, :, ks, rows], z_s.at[n], z_r.at[n], zpeer)

    def z_mid(l, i):
        q, n = turn(i), 8 + l
        ks = pl.ds(0, 1) if i == 0 else pl.ds(0, 2)
        return remote(cs.at[q, l, ks, mid], zr.at[q, l, ks, mid], z_s.at[n], z_r.at[n], zpeer)

    def z_last(n):
        at = 8 + post + n
        l, k = post + n // 2, n % 2
        return remote(cs.at[:, l, k, mid], zr.at[:, l, k, mid], z_s.at[at], z_r.at[at], zpeer)

    def z_mid_all(l):
        size = rb.at[0, pl.ds(0, 7), mid]
        return remote(size, size, z_s.at[8 + l], z_r.at[8 + l], zpeer)

    def three(u, send, recv):
        lv, rows = span(u)
        size = rsr.at[:, lv, rows]
        return remote(size, size, send.at[u], recv.at[u], zpeer)

    def rs_all(u):
        return three(u, rs_s, rs_r)

    def ag_all(u):
        return three(u, ag_s, ag_r)

    def pre_all(send, recv):
        return remote(pr, pr, send, recv, zpeer)

    ref_part = ((pl.ds(0, post), pl.ds(8, 8)), (pl.ds(0, half), pl.ds(32, 16)), (pl.ds(0, post), pl.ds(16, 16)))

    def ref_copy(s, i):
        lv, rows = ref_part[s]
        return remote(
            cs.at[mb, lv, 1, rows], rb.at[mb, lv, rows], ref_s.at[s, i - 1], ref_r.at[s, i - 1], ypeer(4 - i)
        )

    def ref_arrival(s, i):
        lv, rows = ref_part[s]
        here = rb.at[turn(i), lv, rows]
        return remote(here, here, ref_s.at[s, i - 1], ref_r.at[s, i - 1], zpeer)

    def span(u):
        if isinstance(u, int) and u < 2:
            return pl.ds(0, half), pl.ds(40 * u, 8)
        return pl.ds(u - 2, 1), mid

    def rs_copy(u, i):
        lv, rows = span(u)
        q = turn(i)
        return remote(ps.at[q, lv, rows], rsr.at[i - 1, lv, rows], rs_s.at[u], rs_r.at[u], ypeer(i))

    def ag_copy(u, i):
        lv, rows = span(u)
        here = sg.at[mb, lv, rows]
        return remote(here, here, ag_s.at[u], ag_r.at[u], ypeer(i))

    def pre_rs(i):
        return remote(pp.at[turn(i)], pr.at[i - 1], pre_rs_s, pre_rs_r, ypeer(i))

    def pre_ag(i):
        return remote(pg.at[mb], pg.at[mb], pre_ag_s, pre_ag_r, ypeer(i))

    def k_up():
        return remote(kp.at[pl.ds(8, 8)], kp.at[pl.ds(56, 8)], h_s.at[0], h_r.at[0], up)

    def k_down():
        return remote(kp.at[pl.ds(48, 8)], kp.at[pl.ds(0, 8)], h_s.at[1], h_r.at[1], down)

    def f_up():
        return remote(hst, hrb, h_s.at[2], h_r.at[2], up)

    def f_down():
        return remote(hsb, hrt, h_s.at[3], h_r.at[3], down)

    def f_up_part(p):
        lv = pl.ds(2 * p, 2)
        if p == 0:
            return remote(hst.at[lv], hrb.at[lv], h_s.at[2], h_r.at[2], up)
        if p == parts - 1:
            return remote(hst.at[lv], hrb.at[lv], part_s.at[p - 1], part_r.at[p - 1], up)
        return remote(hst.at[lv], hrelay, part_s.at[p - 1], part_r.at[3], upper(p))

    def f_down_part(p):
        lv = pl.ds(2 * p, 2)
        if p == 0:
            return remote(hsb.at[lv], hrt.at[lv], h_s.at[3], h_r.at[3], down)
        if p == parts - 1:
            return remote(hsb.at[lv], hrt.at[lv], part_s.at[p - 1], part_r.at[p - 1], down)
        return remote(hsb.at[lv], hrelay, part_s.at[p - 1], part_r.at[3], lower(p))

    def relay_up():
        dst = hrb.at[pl.ds(2 * turn_of, 2)]
        return remote(hrelay, dst, relay_s, part_r.at[turn_of - 1], upper(0))

    def relay_down():
        dst = hrt.at[pl.ds(2 * turn_of, 2)]
        return remote(hrelay, dst, relay_s, part_r.at[turn_of - 1], lower(0))

    def part_arrival(dst, p):
        here = dst.at[pl.ds(2 * p, 2)]
        return remote(here, here, part_s.at[p - 1], part_r.at[p - 1], zpeer)

    def pass_on():
        @pl.when(is_relay)
        def _():
            remote(hrelay, hrelay, relay_s, part_r.at[3], zpeer).wait_recv()

            @pl.when(st < cut)
            def _():
                relay_up().start()

            @pl.when(st > cut)
            def _():
                relay_down().start()

    def parts_arrive():
        @pl.when(over)
        def _():
            for p in range(1, parts):
                part_arrival(hrb, p).wait_recv()

        @pl.when(under)
        def _():
            for p in range(1, parts):
                part_arrival(hrt, p).wait_recv()

    def products(s, i):
        j, q = 4 * s + i, turn(i)
        rows = pl.ds(block_rows[s], 16)
        own = half * tm
        other = half - own

        def tile(n, c):
            k = lax.rem(n, 2)
            lanes = pl.ds(pl.multiple_of((n // 2) * LANES, LANES), LANES)
            part = [
                mv[j, 0, k, m, :, lanes].astype(f32) * gv[j, 0, m, :, lanes]
                + mv[j, 1, k, m, :, lanes].astype(f32) * gv[j, 1, m, :, lanes]
                for m in range(levels)
            ]
            for start, dst in ((other, cs), (own, co)):
                for l in range(half):
                    total = vertical[0, start + l] * part[0]
                    for m in range(1, levels):
                        total = total + vertical[m, start + l] * part[m]
                    dst[q, l, k, rows, lanes] = total
            return c

        lax.fori_loop(0, 2 * tiles, tile, 0)

    ref_tiles = (((8, post),), ((32, post), (40, half)), ((16, post), (24, post)))

    def subtract(s, q, refer, ks):
        for r, count in ref_tiles[s]:
            rows = pl.ds(r, 8)

            def sub(l, c):
                ref = refer(l, rows)
                for k in ks:
                    cs[q, l, k, rows] = cs[q, l, k, rows] - ref
                return c

            lax.fori_loop(0, count, sub, 0)

    def mix(s, i):
        for copy in loads(s, i):
            copy.wait()
        products(s, i)
        if isinstance(i, int) and i == 0:
            if s == 0:
                peers = 4 + has_up.astype(jnp.int32) + has_down.astype(jnp.int32)
                peers = peers + 2 * (parts - 2) * at_cut.astype(jnp.int32) + 2 * is_relay.astype(jnp.int32)
                pl.semaphore_wait(barrier, peers)
            for n in (1, 2, 3):
                ref_copy(s, n).start()
            if s == 0:
                z_edge(0, i).start()
            subtract(s, mb, lambda l, rows: cs[mb, l, 1, rows], (0,))
        elif s == 0:
            z_edge(0, i).start()

    def mix_rest(s, after):
        def step(i, c):
            after(i)
            mix(s, i)
            return c

        lax.fori_loop(1, 4, step, 0)

    def refer(s):
        def step(i, c):
            q = turn(i)
            ref_arrival(s, i).wait_recv()
            subtract(s, q, lambda l, rows: rb[q, l, rows], (0, 1))
            if s == 1:
                z_edge(1, i).start()
            return c

        lax.fori_loop(1, 4, step, 0)

    vload.wait()
    start_loads(0, 2)
    mix(0, 0)
    start_loads(0, 3)
    mix(1, 0)
    mix_rest(0, lambda i: start_loads(1, i))
    z_edge(1, 0).start()
    mix_rest(1, lambda i: start_loads(2, i - 1))
    refer(1)
    start_loads(2, 3)
    mix(2, 0)
    mix_rest(2, lambda i: None)
    refer(0)
    refer(2)

    kload.wait()

    @pl.when(has_up)
    def _():
        k_up().start()

    @pl.when(has_down)
    def _():
        k_down().start()

    @pl.when(jnp.logical_not(has_up))
    def _():
        kp[pl.ds(0, 8)] = jnp.zeros((8, kp.shape[1]), f32)
        hrt[...] = jnp.zeros(hrt.shape, f32)

    @pl.when(jnp.logical_not(has_down))
    def _():
        kp[pl.ds(56, 8)] = jnp.zeros((8, kp.shape[1]), f32)
        hrb[...] = jnp.zeros(hrb.shape, f32)

    def add_up(q, l, rows):
        a = co[q, l, 0, rows] + zr[q, l, 0, rows]
        b = co[q, l, 1, rows] + zr[q, l, 1, rows]
        co[q, l, 0, rows] = a
        co[q, l, 1, rows] = b
        ps[q, l, rows] = a + b

    def arrive_edge(u, i):
        z_edge(u, i).wait_recv()
        q = turn(i)

        def body(l, c):
            add_up(q, l, pl.ds(40 * u, 8))
            return c

        lax.fori_loop(0, half, body, 0)
        if i:
            rs_copy(u, i).start()

    def arrive_mid(l):
        z_mid_all(l).wait_recv()
        for i in range(4):
            add_up(turn(i), l, mid)
            if i:
                rs_copy(2 + l, i).start()

    def total(u):
        lv, rows = span(u)
        rs_all(u).wait_recv()

        def body(l, c):
            sg[mb, l, rows] = (ps[mb, l, rows] + rsr[0, l, rows]) + (rsr[1, l, rows] + rsr[2, l, rows])
            return c

        lax.fori_loop(lv.start, lv.start + lv.size, body, 0)
        for i in (1, 2, 3):
            ag_copy(u, i).start()

    def centred(u):
        lv, rows = span(u)
        ag_all(u).wait_recv()

        def body(l, c):
            for q in range(4):
                mean = sg[q, l, rows] * (1.0 / n_members)
                for k in range(2):
                    out[l, k, rows, pl.ds(q * quarter, quarter)] = (co[q, l, k, rows] - mean) * scale
            return c

        lax.fori_loop(lv.start, lv.start + lv.size, body, 0)

    def pre_sum():
        for n in range(4):
            q = turn(n)

            def add(l, c):
                for h, src in enumerate((cs, co)):
                    pp[q, h, l] = src[q, post + l, 0, mid] + src[q, post + l, 1, mid]
                return c

            lax.fori_loop(0, 2, add, 0)
            if n:
                pre_rs(n).start()

    def pre_total():
        pre_all(pre_rs_s, pre_rs_r).wait_recv()

        def add(l, c):
            for h in range(2):
                pg[mb, h, l] = (pp[mb, h, l] + pr[0, h, l]) + (pr[1, h, l] + pr[2, h, l])
            return c

        lax.fori_loop(0, 2, add, 0)
        for i in (1, 2, 3):
            pre_ag(i).start()

    def pre_centred():
        pre_all(pre_ag_s, pre_ag_r).wait_recv()
        for i in (1, 2, 3):
            ref_copy(1, i).wait_send()

        def centre(q, c):
            for l in range(2):
                for h, dst in enumerate((cs, co)):
                    mean = pg[q, h, l] * (1.0 / n_members)
                    for k in range(2):
                        dst[q, post + l, k, mid] = dst[q, post + l, k, mid] - mean
            return c

        lax.fori_loop(0, 4, centre, 0)

    def arrive_last(n):
        z_last(n).wait_recv()
        l, k = post + n // 2, n % 2
        for q in range(4):
            out[l, k, mid, pl.ds(q * quarter, quarter)] = (co[q, l, k, mid] + zr[q, l, k, mid]) * scale

    def edge_top():
        def body(l, c):
            for k in range(2):
                hst[l, pl.ds(4 * k, 4)] = out[l, k, pl.ds(0, 4)]
            return c

        @pl.when(has_up)
        def _():
            lax.fori_loop(0, half, body, 0)

            @pl.when(under)
            def _():
                for p in range(parts):
                    f_up_part(p).start()

            @pl.when(jnp.logical_not(under))
            def _():
                f_up().start()

    def edge_bottom():
        def body(l, c):
            for k in range(2):
                hsb[l, pl.ds(4 * k, 4)] = out[l, k, pl.ds(44, 4)]
            return c

        @pl.when(has_down)
        def _():
            lax.fori_loop(0, half, body, 0)

            @pl.when(over)
            def _():
                for p in range(parts):
                    f_down_part(p).start()

            @pl.when(jnp.logical_not(over))
            def _():
                f_down().start()

    def smooth(l, ks=(0, 1)):
        for k in ks:
            w[pl.ds(8, 48)] = out[l, k]
            w[pl.ds(4, 4)] = hrt[l, pl.ds(4 * k, 4)]
            w[pl.ds(56, 4)] = hrb[l, pl.ds(4 * k, 4)]

            row = lax.broadcasted_iota(jnp.int32, (8, w.shape[1]), 0)
            top_row, bottom_row = row == 0, row == 7

            def filter_step(n, c):
                def product(t):
                    v[pl.ds(8 * t + 8, 8)] = kp[pl.ds(8 * t, 8)] * w[pl.ds(8 * t, 8)]

                product(0)
                for t in range(8):
                    if t < 7:
                        product(t + 1)
                    before, at, after = (v[pl.ds(8 * t + 8 * n, 8)] for n in range(3))
                    around = pltpu.roll(at, 1, 1) + pltpu.roll(at, at.shape[1] - 1, 1)
                    around = around + pltpu.roll(jnp.where(bottom_row, before, at), 1, 0)
                    around = around + pltpu.roll(jnp.where(top_row, after, at), 7, 0)
                    w[pl.ds(8 * t, 8)] = (w[pl.ds(8 * t, 8)] - 4.0 * at) + around
                return c

            lax.fori_loop(0, NSTEP, filter_step, 0)
            out[l, k] = w[pl.ds(8, 48)]

    def wait_halos():
        @pl.when(has_up)
        def _():
            k_down().wait_recv()

            @pl.when(under)
            def _():
                f_down_part(0).wait_recv()

            @pl.when(jnp.logical_not(under))
            def _():
                f_down().wait_recv()

        @pl.when(has_down)
        def _():
            k_up().wait_recv()

            @pl.when(over)
            def _():
                f_up_part(0).wait_recv()

            @pl.when(jnp.logical_not(over))
            def _():
                f_up().wait_recv()

    w[pl.ds(0, 8)] = jnp.zeros((8, w.shape[1]), f32)
    w[pl.ds(56, 8)] = jnp.zeros((8, w.shape[1]), f32)
    zr[mb, pl.ds(0, post), 1, pl.ds(8, 40)] = jnp.zeros((post, 40, quarter), f32)
    zr[mb, pl.ds(post, 2), 1, pl.ds(40, 8)] = jnp.zeros((2, 8, quarter), f32)
    v[pl.ds(0, 8)] = jnp.zeros((8, v.shape[1]), f32)
    v[pl.ds(72, 8)] = jnp.zeros((8, v.shape[1]), f32)

    def mid_sent(l):
        z_mid_all(l).wait_send()

    def sums_sent(u):
        rs_all(u).wait_send()
        ag_all(u).wait_send()

    def edges_sent():
        @pl.when(is_relay)
        def _():
            remote(hrelay, hrelay, relay_s, part_r.at[3], zpeer).wait_send()

        for u in range(2):
            for i in range(4):
                z_edge(u, i).wait_send()
            sums_sent(u)
        for i in (1, 2, 3):
            ref_copy(0, i).wait_send()
            ref_copy(2, i).wait_send()

        @pl.when(has_up)
        def _():
            k_up().wait_send()

            @pl.when(under)
            def _():
                for p in range(parts):
                    f_up_part(p).wait_send()

            @pl.when(jnp.logical_not(under))
            def _():
                f_up().wait_send()

        @pl.when(has_down)
        def _():
            k_down().wait_send()

            @pl.when(over)
            def _():
                for p in range(parts):
                    f_down_part(p).wait_send()

            @pl.when(jnp.logical_not(over))
            def _():
                f_down().wait_send()

    def start_mid(l):
        for i in range(4):
            z_mid(l, i).start()

    start_mid(0)
    start_mid(1)
    for i in range(4):
        arrive_edge(0, i)
    arrive_edge(1, 0)
    arrive_edge(1, 1)
    total(0)
    start_mid(2)
    arrive_edge(1, 2)
    arrive_edge(1, 3)
    start_mid(3)
    total(1)
    centred(0)
    edge_top()
    pre_sum()
    start_mid(4)
    start_mid(5)
    arrive_mid(0)
    centred(1)
    edge_bottom()
    arrive_mid(1)
    total(2)
    pass_on()
    pre_total()
    arrive_mid(2)
    total(3)
    wait_halos()
    centred(2)
    smooth(0)
    pre_centred()
    for n in range(4):
        z_last(n).start()
    edges_sent()
    parts_arrive()

    def rest(l, c):
        arrive_mid(l)
        total(l + 1)
        centred(l)
        smooth(l - 2)
        mid_sent(l - 3)
        sums_sent(l - 1)
        return c

    lax.fori_loop(3, post, rest, 0)
    total(post + 1)
    centred(post)
    smooth(post - 2)
    arrive_last(0)
    smooth(post, (0,))
    centred(post + 1)
    smooth(post - 1)
    for n in (post - 3, post - 2, post - 1):
        mid_sent(n)
        sums_sent(n + 2)
    arrive_last(1)
    smooth(post, (1,))
    arrive_last(2)
    smooth(post + 1, (0,))
    pre_all(pre_rs_s, pre_rs_r).wait_send()
    pre_all(pre_ag_s, pre_ag_r).wait_send()
    z_last(0).wait_send()
    z_last(1).wait_send()
    arrive_last(3)
    smooth(post + 1, (1,))

    z_last(2).wait_send()
    z_last(3).wait_send()


def body(members, slot_grad, diffusivity, vertical, *, sizes):
    slots, pair, levels, rows, lon = members.shape
    half, quarter = levels // sizes["tm"], lon // 4
    n_members = pair * sizes["member"]
    dma = pltpu.SemaphoreType.DMA
    f32 = jnp.float32
    field = (4, half, pair, rows, quarter)
    one = (4, half, rows, quarter)
    scratch = [
        pltpu.SMEM((levels, levels), f32),
        pltpu.VMEM((4, 2, 2, 32, quarter), f32),
        pltpu.VMEM((3, 2, 2, 32, quarter), f32),
        pltpu.VMEM((4, 2, 2, 32, quarter), f32),
        pltpu.VMEM((12, slots, pair, levels, 16, quarter), members.dtype),
        pltpu.VMEM((12, slots, levels, 16, quarter), f32),
        pltpu.VMEM(field, f32),
        pltpu.VMEM(field, f32),
        pltpu.VMEM(field, f32),
        pltpu.VMEM(one, f32),
        pltpu.VMEM(one, f32),
        pltpu.VMEM((3,) + one[1:], f32),
        pltpu.VMEM(one, f32),
        pltpu.VMEM((64, lon), f32),
        pltpu.VMEM((half, 8, lon), f32),
        pltpu.VMEM((half, 8, lon), f32),
        pltpu.VMEM((half, 8, lon), f32),
        pltpu.VMEM((half, 8, lon), f32),
        pltpu.VMEM((2, 8, lon), f32),
        pltpu.VMEM((64, lon), f32),
        pltpu.VMEM((80, lon), f32),
        dma,
        dma,
        dma,
        dma,
        dma,
        dma((12, 2)),
        dma,
        dma((10 + half,)),
        dma((10 + half,)),
        dma((3, 3)),
        dma((3, 3)),
        dma((half,)),
        dma((half,)),
        dma((half,)),
        dma((half,)),
        dma((4,)),
        dma((4,)),
        dma((3,)),
        dma((4,)),
        dma,
    ]
    hbm = pl.BlockSpec(memory_space=pltpu.HBM)
    return pl.pallas_call(
        functools.partial(
            kernel, n_state=sizes["state"], scale=float(n_members - 1) ** -0.5, n_members=n_members
        ),
        out_shape=pltpu.VMEM((half, pair, rows, lon), f32),
        in_specs=[hbm] * 4,
        out_specs=pl.BlockSpec(memory_space=pltpu.VMEM),
        scratch_shapes=scratch,
        compiler_params=pltpu.CompilerParams(
            collective_id=0, has_side_effects=True, vmem_limit_bytes=VMEM_LIMIT
        ),
    )(members, slot_grad, diffusivity, vertical)


VMEM_LIMIT = 50 * 1024 * 1024


def solution(mesh):
    in_specs = (
        P("tm", "member", None, "state", None),
        P("tm", None, "state", None),
        P("state", None),
        P(),
    )
    out_specs = P("tm", "member", "state", None)
    step = functools.partial(body, sizes=dict(mesh.shape))
    return jax.shard_map(step, mesh=mesh, in_specs=in_specs, out_specs=out_specs, check_vma=False)
```

```python
import functools

import jax
import jax.numpy as jnp
from jax import lax
from jax.experimental import pallas as pl
from jax.experimental.pallas import tpu as pltpu
from jax.sharding import PartitionSpec as P

NSTEP = 4
MESH = pl.DeviceIdType.MESH
LANES = 128


def kernel(
    members, slot_grad, diffusivity, matrix, out,
    vertical, pp, pr, pg, mv, gv, cs, co, zr, rb, ps, rsr, sg, kp, hst, hsb, hrt, hrb, hrelay, w, v,
    v_sem, pre_rs_s, pre_rs_r, pre_ag_s, pre_ag_r, ld_sem, kp_sem, z_s, z_r, ref_s, ref_r, rs_s, rs_r, ag_s, ag_r, h_s, h_r, part_s, part_r, relay_s,
    *, n_state, scale, n_members,
):
    f32 = jnp.float32
    tm, mb, st = lax.axis_index("tm"), lax.axis_index("member"), lax.axis_index("state")
    levels = mv.shape[3]
    half = levels // 2
    post = half - 2
    mid = pl.ds(8, 32)
    quarter = mv.shape[-1]
    tiles = quarter // LANES
    zpeer = (1 - tm, mb, st)
    up, down = (tm, mb, st - 1), (tm, mb, st + 1)
    has_up, has_down = st > 0, st < n_state - 1
    cut = n_state // 2
    parts, share = 3, hrelay.shape[0]
    over, under = st == cut - 1, st == cut
    at_cut = jnp.logical_or(over, under)
    hop = jnp.where(st < cut, cut - 1 - st, st - cut)
    is_relay = jnp.logical_and(lax.rem(hop, 2) == 0, jnp.logical_and(hop > 0, hop < 2 * parts))
    turn_of = hop // 2

    def lower(p):
        return (tm, mb, cut + 2 * p)

    def upper(p):
        return (tm, mb, cut - 1 - 2 * p)

    def turn(i):
        return lax.rem(mb + i, 4)

    def ypeer(i):
        return (tm, turn(i), st)

    def remote(src, dst, send, recv, peer):
        return pltpu.make_async_remote_copy(
            src_ref=src, dst_ref=dst, send_sem=send, recv_sem=recv, device_id=peer, device_id_type=MESH
        )

    block_rows = (0, 32, 16)

    def loads(s, i):
        rows = pl.ds(block_rows[s], 16)
        lanes = pl.ds(pl.multiple_of(turn(i) * quarter, LANES), quarter)
        j = 4 * s + i
        if isinstance(i, int) and i == 0:
            place = (0, 1, 8)[s]
        else:
            place = (i + 1, i + 4, i + 8)[s]
        slot = lax.rem(place, 4)
        return (
            pltpu.make_async_copy(members.at[:, :, :, rows, lanes], mv.at[j], ld_sem.at[slot, 0]),
            pltpu.make_async_copy(slot_grad.at[:, :, rows, lanes], gv.at[j], ld_sem.at[slot, 1]),
        )

    def start_loads(s, i):
        for copy in loads(s, i):
            copy.start()

    vload = pltpu.make_async_copy(matrix, vertical, v_sem)
    vload.start()
    start_loads(0, 0)
    start_loads(1, 0)

    barrier = pltpu.get_barrier_semaphore()
    pl.semaphore_signal(barrier, inc=1, device_id=zpeer, device_id_type=MESH)
    for i in (1, 2, 3):
        pl.semaphore_signal(barrier, inc=1, device_id=ypeer(i), device_id_type=MESH)

    @pl.when(at_cut)
    def _():
        for p in range(1, parts):
            pl.semaphore_signal(barrier, inc=1, device_id=lower(p), device_id_type=MESH)
            pl.semaphore_signal(barrier, inc=1, device_id=upper(p), device_id_type=MESH)

    @pl.when(is_relay)
    def _():
        pl.semaphore_signal(barrier, inc=1, device_id=lower(0), device_id_type=MESH)
        pl.semaphore_signal(barrier, inc=1, device_id=upper(0), device_id_type=MESH)

    @pl.when(has_up)
    def _():
        pl.semaphore_signal(barrier, inc=1, device_id=up, device_id_type=MESH)

    @pl.when(has_down)
    def _():
        pl.semaphore_signal(barrier, inc=1, device_id=down, device_id_type=MESH)

    kload = pltpu.make_async_copy(diffusivity, kp.at[pl.ds(8, 48)], kp_sem)
    kload.start()
    start_loads(0, 1)

    def z_edge(u, i):
        q, rows = turn(i), pl.ds(40 * u, 8)
        ks = pl.ds(0, 1 if u == 1 and isinstance(i, int) and i == 0 else 2)
        n = 4 * u + i
        return remote(cs.at[q, :, ks, rows], zr.at[q, :, ks, rows], z_s.at[n], z_r.at[n], zpeer)

    def z_mid(l, i):
        q, n = turn(i), 8 + l
        ks = pl.ds(0, 1) if i == 0 else pl.ds(0, 2)
        return remote(cs.at[q, l, ks, mid], zr.at[q, l, ks, mid], z_s.at[n], z_r.at[n], zpeer)

    def z_last(n):
        at = 8 + post + n
        l, k = post + n // 2, n % 2
        return remote(cs.at[:, l, k, mid], zr.at[:, l, k, mid], z_s.at[at], z_r.at[at], zpeer)

    def z_mid_all(l):
        size = rb.at[0, pl.ds(0, 7), mid]
        return remote(size, size, z_s.at[8 + l], z_r.at[8 + l], zpeer)

    def three(u, send, recv):
        lv, rows = span(u)
        size = rsr.at[:, lv, rows]
        return remote(size, size, send.at[u], recv.at[u], zpeer)

    def rs_all(u):
        return three(u, rs_s, rs_r)

    def ag_all(u):
        return three(u, ag_s, ag_r)

    def pre_all(send, recv):
        return remote(pr, pr, send, recv, zpeer)

    ref_part = ((pl.ds(0, post), pl.ds(8, 8)), (pl.ds(0, half), pl.ds(32, 16)), (pl.ds(0, post), pl.ds(16, 16)))

    def ref_copy(s, i):
        lv, rows = ref_part[s]
        return remote(
            cs.at[mb, lv, 1, rows], rb.at[mb, lv, rows], ref_s.at[s, i - 1], ref_r.at[s, i - 1], ypeer(4 - i)
        )

    def ref_arrival(s, i):
        lv, rows = ref_part[s]
        here = rb.at[turn(i), lv, rows]
        return remote(here, here, ref_s.at[s, i - 1], ref_r.at[s, i - 1], zpeer)

    def span(u):
        if isinstance(u, int) and u < 2:
            return pl.ds(0, half), pl.ds(40 * u, 8)
        return pl.ds(u - 2, 1), mid

    def rs_copy(u, i):
        lv, rows = span(u)
        q = turn(i)
        return remote(ps.at[q, lv, rows], rsr.at[i - 1, lv, rows], rs_s.at[u], rs_r.at[u], ypeer(i))

    def ag_copy(u, i):
        lv, rows = span(u)
        here = sg.at[mb, lv, rows]
        return remote(here, here, ag_s.at[u], ag_r.at[u], ypeer(i))

    def pre_rs(i):
        return remote(pp.at[turn(i)], pr.at[i - 1], pre_rs_s, pre_rs_r, ypeer(i))

    def pre_ag(i):
        return remote(pg.at[mb], pg.at[mb], pre_ag_s, pre_ag_r, ypeer(i))

    def k_up():
        return remote(kp.at[pl.ds(8, 8)], kp.at[pl.ds(56, 8)], h_s.at[0], h_r.at[0], up)

    def k_down():
        return remote(kp.at[pl.ds(48, 8)], kp.at[pl.ds(0, 8)], h_s.at[1], h_r.at[1], down)

    def f_up():
        return remote(hst, hrb, h_s.at[2], h_r.at[2], up)

    def f_down():
        return remote(hsb, hrt, h_s.at[3], h_r.at[3], down)

    def part_levels(p):
        first = half - share * (parts - 1)
        if isinstance(p, int) and p == 0:
            return pl.ds(0, first)
        return pl.ds(first + share * (p - 1), share)

    def f_up_part(p):
        lv = part_levels(p)
        if p == 0:
            return remote(hst.at[lv], hrb.at[lv], h_s.at[2], h_r.at[2], up)
        return remote(hst.at[lv], hrelay, part_s.at[p - 1], part_r.at[3], upper(p))

    def f_down_part(p):
        lv = part_levels(p)
        if p == 0:
            return remote(hsb.at[lv], hrt.at[lv], h_s.at[3], h_r.at[3], down)
        return remote(hsb.at[lv], hrelay, part_s.at[p - 1], part_r.at[3], lower(p))

    def relay_up():
        dst = hrb.at[part_levels(turn_of)]
        return remote(hrelay, dst, relay_s, part_r.at[turn_of - 1], upper(0))

    def relay_down():
        dst = hrt.at[part_levels(turn_of)]
        return remote(hrelay, dst, relay_s, part_r.at[turn_of - 1], lower(0))

    def part_arrival(dst, p):
        here = dst.at[part_levels(p)]
        return remote(here, here, part_s.at[p - 1], part_r.at[p - 1], zpeer)

    def pass_on():
        @pl.when(is_relay)
        def _():
            remote(hrelay, hrelay, relay_s, part_r.at[3], zpeer).wait_recv()

            @pl.when(st < cut)
            def _():
                relay_up().start()

            @pl.when(st > cut)
            def _():
                relay_down().start()

    def parts_arrive():
        @pl.when(over)
        def _():
            for p in range(1, parts):
                part_arrival(hrb, p).wait_recv()

        @pl.when(under)
        def _():
            for p in range(1, parts):
                part_arrival(hrt, p).wait_recv()

    def products(s, i):
        j, q = 4 * s + i, turn(i)
        rows = pl.ds(block_rows[s], 16)
        own = half * tm
        other = half - own

        def tile(n, c):
            k = lax.rem(n, 2)
            lanes = pl.ds(pl.multiple_of((n // 2) * LANES, LANES), LANES)
            part = [
                mv[j, 0, k, m, :, lanes].astype(f32) * gv[j, 0, m, :, lanes]
                + mv[j, 1, k, m, :, lanes].astype(f32) * gv[j, 1, m, :, lanes]
                for m in range(levels)
            ]
            for start, dst in ((other, cs), (own, co)):
                for l in range(half):
                    total = vertical[0, start + l] * part[0]
                    for m in range(1, levels):
                        total = total + vertical[m, start + l] * part[m]
                    dst[q, l, k, rows, lanes] = total
            return c

        lax.fori_loop(0, 2 * tiles, tile, 0)

    ref_tiles = (((8, post),), ((32, post), (40, half)), ((16, post), (24, post)))

    def subtract(s, q, refer, ks):
        for r, count in ref_tiles[s]:
            rows = pl.ds(r, 8)

            def sub(l, c):
                ref = refer(l, rows)
                for k in ks:
                    cs[q, l, k, rows] = cs[q, l, k, rows] - ref
                return c

            lax.fori_loop(0, count, sub, 0)

    def mix(s, i):
        for copy in loads(s, i):
            copy.wait()
        products(s, i)
        if isinstance(i, int) and i == 0:
            if s == 0:
                peers = 4 + has_up.astype(jnp.int32) + has_down.astype(jnp.int32)
                peers = peers + 2 * (parts - 1) * at_cut.astype(jnp.int32) + 2 * is_relay.astype(jnp.int32)
                pl.semaphore_wait(barrier, peers)
            if s == 0:
                z_edge(0, i).start()
            else:
                for at in (1, 0) if s == 1 else (2,):
                    for n in (1, 2, 3):
                        ref_copy(at, n).start()
            subtract(s, mb, lambda l, rows: cs[mb, l, 1, rows], (0,))
        elif s == 0:
            z_edge(0, i).start()

    def mix_rest(s, after):
        def step(i, c):
            after(i)
            mix(s, i)
            return c

        lax.fori_loop(1, 4, step, 0)

    def refer(s):
        def step(i, c):
            q = turn(i)
            ref_arrival(s, i).wait_recv()
            subtract(s, q, lambda l, rows: rb[q, l, rows], (0, 1))
            if s == 1:
                z_edge(1, i).start()
            return c

        lax.fori_loop(1, 4, step, 0)

    vload.wait()
    start_loads(0, 2)
    mix(0, 0)
    start_loads(0, 3)
    mix(1, 0)
    mix_rest(0, lambda i: start_loads(1, i))
    z_edge(1, 0).start()
    mix_rest(1, lambda i: start_loads(2, i - 1))
    refer(1)
    start_loads(2, 3)
    mix(2, 0)
    mix_rest(2, lambda i: None)
    refer(0)
    refer(2)

    kload.wait()

    @pl.when(has_up)
    def _():
        k_up().start()

    @pl.when(has_down)
    def _():
        k_down().start()

    @pl.when(jnp.logical_not(has_up))
    def _():
        kp[pl.ds(0, 8)] = jnp.zeros((8, kp.shape[1]), f32)
        hrt[...] = jnp.zeros(hrt.shape, f32)

    @pl.when(jnp.logical_not(has_down))
    def _():
        kp[pl.ds(56, 8)] = jnp.zeros((8, kp.shape[1]), f32)
        hrb[...] = jnp.zeros(hrb.shape, f32)

    def add_up(q, l, rows):
        a = co[q, l, 0, rows] + zr[q, l, 0, rows]
        b = co[q, l, 1, rows] + zr[q, l, 1, rows]
        co[q, l, 0, rows] = a
        co[q, l, 1, rows] = b
        ps[q, l, rows] = a + b

    def arrive_edge(u, i):
        z_edge(u, i).wait_recv()
        q = turn(i)

        def body(l, c):
            add_up(q, l, pl.ds(40 * u, 8))
            return c

        lax.fori_loop(0, half, body, 0)
        if i:
            rs_copy(u, i).start()

    def arrive_mid(l):
        z_mid_all(l).wait_recv()
        for i in range(4):
            add_up(turn(i), l, mid)
            if i:
                rs_copy(2 + l, i).start()

    def total(u):
        lv, rows = span(u)
        rs_all(u).wait_recv()

        def body(l, c):
            sg[mb, l, rows] = (ps[mb, l, rows] + rsr[0, l, rows]) + (rsr[1, l, rows] + rsr[2, l, rows])
            return c

        lax.fori_loop(lv.start, lv.start + lv.size, body, 0)
        for i in (1, 2, 3):
            ag_copy(u, i).start()

    def centred(u):
        lv, rows = span(u)
        ag_all(u).wait_recv()

        def body(l, c):
            for q in range(4):
                mean = sg[q, l, rows] * (1.0 / n_members)
                for k in range(2):
                    out[l, k, rows, pl.ds(q * quarter, quarter)] = (co[q, l, k, rows] - mean) * scale
            return c

        lax.fori_loop(lv.start, lv.start + lv.size, body, 0)

    def pre_sum():
        for n in range(4):
            q = turn(n)

            def add(l, c):
                for h, src in enumerate((cs, co)):
                    pp[q, h, l] = src[q, post + l, 0, mid] + src[q, post + l, 1, mid]
                return c

            lax.fori_loop(0, 2, add, 0)
            if n:
                pre_rs(n).start()

    def pre_total():
        pre_all(pre_rs_s, pre_rs_r).wait_recv()

        def add(l, c):
            for h in range(2):
                pg[mb, h, l] = (pp[mb, h, l] + pr[0, h, l]) + (pr[1, h, l] + pr[2, h, l])
            return c

        lax.fori_loop(0, 2, add, 0)
        for i in (1, 2, 3):
            pre_ag(i).start()

    def pre_centred():
        pre_all(pre_ag_s, pre_ag_r).wait_recv()
        for i in (1, 2, 3):
            ref_copy(1, i).wait_send()

        def centre(q, c):
            for l in range(2):
                for h, dst in enumerate((cs, co)):
                    mean = pg[q, h, l] * (1.0 / n_members)
                    for k in range(2):
                        dst[q, post + l, k, mid] = dst[q, post + l, k, mid] - mean
            return c

        lax.fori_loop(0, 4, centre, 0)

    def arrive_last(n):
        z_last(n).wait_recv()
        l, k = post + n // 2, n % 2
        for q in range(4):
            out[l, k, mid, pl.ds(q * quarter, quarter)] = (co[q, l, k, mid] + zr[q, l, k, mid]) * scale

    def edge_top():
        def body(l, c):
            for k in range(2):
                hst[l, pl.ds(4 * k, 4)] = out[l, k, pl.ds(0, 4)]
            return c

        @pl.when(has_up)
        def _():
            lax.fori_loop(0, half, body, 0)

            @pl.when(under)
            def _():
                for p in range(parts):
                    f_up_part(p).start()

            @pl.when(jnp.logical_not(under))
            def _():
                f_up().start()

    def edge_bottom():
        def body(l, c):
            for k in range(2):
                hsb[l, pl.ds(4 * k, 4)] = out[l, k, pl.ds(44, 4)]
            return c

        @pl.when(has_down)
        def _():
            lax.fori_loop(0, half, body, 0)

            @pl.when(over)
            def _():
                for p in range(parts):
                    f_down_part(p).start()

            @pl.when(jnp.logical_not(over))
            def _():
                f_down().start()

    def smooth(l, ks=(0, 1)):
        for k in ks:
            w[pl.ds(8, 48)] = out[l, k]
            w[pl.ds(4, 4)] = hrt[l, pl.ds(4 * k, 4)]
            w[pl.ds(56, 4)] = hrb[l, pl.ds(4 * k, 4)]

            row = lax.broadcasted_iota(jnp.int32, (8, w.shape[1]), 0)
            top_row, bottom_row = row == 0, row == 7

            def filter_step(n, c):
                def product(t):
                    v[pl.ds(8 * t + 8, 8)] = kp[pl.ds(8 * t, 8)] * w[pl.ds(8 * t, 8)]

                product(0)
                for t in range(8):
                    if t < 7:
                        product(t + 1)
                    before, at, after = (v[pl.ds(8 * t + 8 * n, 8)] for n in range(3))
                    around = pltpu.roll(at, 1, 1) + pltpu.roll(at, at.shape[1] - 1, 1)
                    around = around + pltpu.roll(jnp.where(bottom_row, before, at), 1, 0)
                    around = around + pltpu.roll(jnp.where(top_row, after, at), 7, 0)
                    w[pl.ds(8 * t, 8)] = (w[pl.ds(8 * t, 8)] - 4.0 * at) + around
                return c

            lax.fori_loop(0, NSTEP, filter_step, 0)
            out[l, k] = w[pl.ds(8, 48)]

    def wait_halos():
        @pl.when(has_up)
        def _():
            k_down().wait_recv()

            @pl.when(under)
            def _():
                f_down_part(0).wait_recv()

            @pl.when(jnp.logical_not(under))
            def _():
                f_down().wait_recv()

        @pl.when(has_down)
        def _():
            k_up().wait_recv()

            @pl.when(over)
            def _():
                f_up_part(0).wait_recv()

            @pl.when(jnp.logical_not(over))
            def _():
                f_up().wait_recv()

    w[pl.ds(0, 8)] = jnp.zeros((8, w.shape[1]), f32)
    w[pl.ds(56, 8)] = jnp.zeros((8, w.shape[1]), f32)
    zr[mb, pl.ds(0, post), 1, pl.ds(8, 40)] = jnp.zeros((post, 40, quarter), f32)
    zr[mb, pl.ds(post, 2), 1, pl.ds(40, 8)] = jnp.zeros((2, 8, quarter), f32)
    v[pl.ds(0, 8)] = jnp.zeros((8, v.shape[1]), f32)
    v[pl.ds(72, 8)] = jnp.zeros((8, v.shape[1]), f32)

    def mid_sent(l):
        z_mid_all(l).wait_send()

    def sums_sent(u):
        rs_all(u).wait_send()
        ag_all(u).wait_send()

    def edges_sent():
        @pl.when(is_relay)
        def _():
            remote(hrelay, hrelay, relay_s, part_r.at[3], zpeer).wait_send()

        for u in range(2):
            for i in range(4):
                z_edge(u, i).wait_send()
            sums_sent(u)
        for i in (1, 2, 3):
            ref_copy(0, i).wait_send()
            ref_copy(2, i).wait_send()

        @pl.when(has_up)
        def _():
            k_up().wait_send()

            @pl.when(under)
            def _():
                for p in range(parts):
                    f_up_part(p).wait_send()

            @pl.when(jnp.logical_not(under))
            def _():
                f_up().wait_send()

        @pl.when(has_down)
        def _():
            k_down().wait_send()

            @pl.when(over)
            def _():
                for p in range(parts):
                    f_down_part(p).wait_send()

            @pl.when(jnp.logical_not(over))
            def _():
                f_down().wait_send()

    def start_mid(l):
        for i in range(4):
            z_mid(l, i).start()

    start_mid(0)
    start_mid(1)
    for i in range(4):
        arrive_edge(0, i)
    arrive_edge(1, 0)
    arrive_edge(1, 1)
    total(0)
    start_mid(2)
    arrive_edge(1, 2)
    arrive_edge(1, 3)
    start_mid(3)
    total(1)
    centred(0)
    edge_top()
    pre_sum()
    start_mid(4)
    start_mid(5)
    arrive_mid(0)
    centred(1)
    edge_bottom()
    arrive_mid(1)
    total(2)
    pass_on()
    pre_total()
    arrive_mid(2)
    total(3)
    wait_halos()
    centred(2)
    smooth(0)
    pre_centred()
    for n in range(4):
        z_last(n).start()
    edges_sent()
    parts_arrive()

    def rest(l, c):
        arrive_mid(l)
        total(l + 1)
        centred(l)
        smooth(l - 2)
        mid_sent(l - 3)
        sums_sent(l - 1)
        return c

    lax.fori_loop(3, post, rest, 0)
    total(post + 1)
    centred(post)
    smooth(post - 2)
    arrive_last(0)
    smooth(post, (0,))
    centred(post + 1)
    smooth(post - 1)
    for n in (post - 3, post - 2, post - 1):
        mid_sent(n)
        sums_sent(n + 2)
    arrive_last(1)
    smooth(post, (1,))
    arrive_last(2)
    smooth(post + 1, (0,))
    pre_all(pre_rs_s, pre_rs_r).wait_send()
    pre_all(pre_ag_s, pre_ag_r).wait_send()
    z_last(0).wait_send()
    z_last(1).wait_send()
    arrive_last(3)
    smooth(post + 1, (1,))

    z_last(2).wait_send()
    z_last(3).wait_send()


def body(members, slot_grad, diffusivity, vertical, *, sizes):
    slots, pair, levels, rows, lon = members.shape
    half, quarter = levels // sizes["tm"], lon // 4
    n_members = pair * sizes["member"]
    dma = pltpu.SemaphoreType.DMA
    f32 = jnp.float32
    field = (4, half, pair, rows, quarter)
    one = (4, half, rows, quarter)
    scratch = [
        pltpu.SMEM((levels, levels), f32),
        pltpu.VMEM((4, 2, 2, 32, quarter), f32),
        pltpu.VMEM((3, 2, 2, 32, quarter), f32),
        pltpu.VMEM((4, 2, 2, 32, quarter), f32),
        pltpu.VMEM((12, slots, pair, levels, 16, quarter), members.dtype),
        pltpu.VMEM((12, slots, levels, 16, quarter), f32),
        pltpu.VMEM(field, f32),
        pltpu.VMEM(field, f32),
        pltpu.VMEM(field, f32),
        pltpu.VMEM(one, f32),
        pltpu.VMEM(one, f32),
        pltpu.VMEM((3,) + one[1:], f32),
        pltpu.VMEM(one, f32),
        pltpu.VMEM((64, lon), f32),
        pltpu.VMEM((half, 8, lon), f32),
        pltpu.VMEM((half, 8, lon), f32),
        pltpu.VMEM((half, 8, lon), f32),
        pltpu.VMEM((half, 8, lon), f32),
        pltpu.VMEM((3, 8, lon), f32),
        pltpu.VMEM((64, lon), f32),
        pltpu.VMEM((80, lon), f32),
        dma,
        dma,
        dma,
        dma,
        dma,
        dma((4, 2)),
        dma,
        dma((10 + half,)),
        dma((10 + half,)),
        dma((3, 3)),
        dma((3, 3)),
        dma((half,)),
        dma((half,)),
        dma((half,)),
        dma((half,)),
        dma((4,)),
        dma((4,)),
        dma((3,)),
        dma((4,)),
        dma,
    ]
    hbm = pl.BlockSpec(memory_space=pltpu.HBM)
    return pl.pallas_call(
        functools.partial(
            kernel, n_state=sizes["state"], scale=float(n_members - 1) ** -0.5, n_members=n_members
        ),
        out_shape=pltpu.VMEM((half, pair, rows, lon), f32),
        in_specs=[hbm] * 4,
        out_specs=pl.BlockSpec(memory_space=pltpu.VMEM),
        scratch_shapes=scratch,
        compiler_params=pltpu.CompilerParams(
            collective_id=0, has_side_effects=True, vmem_limit_bytes=VMEM_LIMIT
        ),
    )(members, slot_grad, diffusivity, vertical)


VMEM_LIMIT = 50 * 1024 * 1024


def solution(mesh):
    in_specs = (
        P("tm", "member", None, "state", None),
        P("tm", None, "state", None),
        P("state", None),
        P(),
    )
    out_specs = P("tm", "member", "state", None)
    step = functools.partial(body, sizes=dict(mesh.shape))
    return jax.shard_map(step, mesh=mesh, in_specs=in_specs, out_specs=out_specs, check_vma=False)
```
